32 devices in a mesh: row: 4 (over z), col: 8 (over y, x, core).
Axes of the slice: x: 2, y: 2, z: 4, core: 2. Of those that a mesh axis runs over, the one named last changes fastest.
Arguments:
- a_matrix: bfloat16 [8192, 8192], P('row', 'col'), may hold values from -6 to 6
- a_flags: int32 [64, 64], P('row', 'col'), may hold values from 0 to 1, as said below
- b_matrix: bfloat16 [8192, 16384], P('row', 'col'), may hold values from -0.1875 to 0.1875
- b_flags: int32 [64, 128], P('row', 'col'), may hold values from 0 to 1, as said below
- sections: int32 [2], replicated, may hold values from 0 to 7
Outputs:
- packed: bfloat16 [8192, 16384], P('row', 'col')
- tile_place: int32 [64, 128], P('row', 'col')
The draws below stay inside these ranges and needn't reach their ends.
Inputs may be any that keep to these rules, and one draw needn't show every extreme that they name: `a_flags`: 0 or 1; the 16 x 8 tiles of one device hold at most 64 ones, and some device holds exactly 64. `b_flags`: 0 or 1; each aligned block of 8 x 16 tiles holds at most 64 ones, and some block exactly 64.
All inputs are finite; a program needn't handle non-finite values.
Results may differ from the reference program's by a relative error of at most 0.001.
Values may be sent and summed in bfloat16 or wider, within the bound.
A program may use at most 128 MiB of HBM per device.

```python
import jax
import jax.numpy as jnp
from jax import lax

TILE = 128
TM_DEV = 16
TN_DEV = 16
KT = 8
SECTIONS = 2
MOST = 64
N_ROW = 4
N_COL = 8


def block_flags(key, row_blocks, col_blocks, block_rows, block_cols, ceiling):
    number = row_blocks * col_blocks
    per_block = block_rows * block_cols
    first, second, third = jax.random.split(key, 3)
    counts = jax.random.randint(first, (number,), max(1, ceiling // 4), ceiling + 1)
    chosen = jax.random.randint(second, (), 0, number)
    counts = jnp.where(jnp.arange(number) == chosen, ceiling, counts)
    scores = jax.random.randint(third, (number, per_block), 0, 1 << 20) * per_block + jnp.arange(per_block)[None, :]
    order = jnp.argsort(scores, axis=1, stable=True)
    ranking = jnp.argsort(order, axis=1, stable=True)
    flags = (ranking < counts[:, None]).astype(jnp.int32)
    flags = flags.reshape(row_blocks, col_blocks, block_rows, block_cols).transpose(0, 2, 1, 3)
    return flags.reshape(row_blocks * block_rows, col_blocks * block_cols)


def draw_a_flags(key, part):
    return block_flags(jax.random.fold_in(key, 11), N_ROW, N_COL, TM_DEV, KT, MOST)


def draw_b_flags(key, part):
    return block_flags(jax.random.fold_in(key, 23), N_COL, N_COL, KT, TN_DEV, MOST)


def steps_of(own_key, shape, cuts, smallest, largest):
    factor_of, own = 1.0, jax.random.fold_in(own_key, 6)
    for dim, shards_of in cuts:
        heights = jnp.exp(jax.random.uniform(jax.random.fold_in(own, dim), (shards_of,), jnp.float32, smallest / len(cuts), largest / len(cuts)))
        factor_of = factor_of * jnp.repeat(heights, shape[dim] // shards_of).reshape([-1 if axis == dim else 1 for axis in range(len(shape))])
    return factor_of


def centred(own_key, shape, width, limit, cuts=(), held_as=jnp.bfloat16):
    drawn = width * jax.random.normal(own_key, shape, jnp.float32)
    if cuts:
        drawn = drawn * steps_of(own_key, shape, cuts, -0.22, 0.18)
    return jnp.clip(drawn, -limit, limit).astype(held_as)


def setup_inputs(seed: int = 0) -> dict:
    keys = jax.random.split(jax.random.key(seed), 6)
    a_matrix = centred(keys[0], (TILE * TM_DEV * N_ROW, TILE * KT * N_COL), 1.0, 6.0, ((0, 4), (1, 8)))
    a_flags = draw_a_flags(jax.random.fold_in(keys[5], 71), 0)
    b_matrix = centred(keys[2], (TILE * KT * N_COL, TILE * TN_DEV * N_COL), (KT * TILE) ** -0.5, 0.1875, ((0, 4), (1, 8)))
    b_flags = draw_b_flags(jax.random.fold_in(keys[5], 71), 0)
    sections = jax.random.randint(keys[4], (SECTIONS,), 0, N_COL).astype(jnp.int32)
    return {"a_matrix": a_matrix, "a_flags": a_flags, "b_matrix": b_matrix, "b_flags": b_flags, "sections": sections}


def mask_tiles(matrix, flags, tile_rows, tile_cols):
    shaped = matrix.reshape(tile_rows, TILE, tile_cols, TILE)
    shaped = shaped * flags.astype(matrix.dtype)[:, None, :, None]
    return shaped.reshape(tile_rows * TILE, tile_cols * TILE)


def to_tiles(matrix, tile_rows, tile_cols):
    return matrix.reshape(tile_rows, TILE, tile_cols, TILE).transpose(0, 2, 1, 3).reshape(tile_rows * tile_cols, TILE, TILE)


def from_tiles(tiles, tile_rows, tile_cols):
    return tiles.reshape(tile_rows, tile_cols, TILE, TILE).transpose(0, 2, 1, 3).reshape(tile_rows * TILE, tile_cols * TILE)


def compact(tiles, flags_flat, capacity):
    rank_of = jnp.cumsum(flags_flat) - 1
    slot_ids = jnp.arange(capacity, dtype=jnp.int32)
    matched = (flags_flat[None, :] == 1) & (rank_of[None, :] == slot_ids[:, None])
    source = jnp.sum(jnp.where(matched, jnp.arange(flags_flat.shape[0], dtype=jnp.int32)[None, :], 0), axis=1).astype(jnp.int32)
    is_valid = jnp.any(matched, axis=1)
    return jnp.take(tiles, source, axis=0) * is_valid.astype(tiles.dtype)[:, None, None]


def reference(a_matrix, a_flags, b_matrix, b_flags, sections):
    panel_width = KT * TILE

    def one_block(block):
        row_index = (block // N_COL).astype(jnp.int32)
        col_index = (block % N_COL).astype(jnp.int32)
        product = jnp.zeros((TM_DEV * TILE, TN_DEV * TILE), jnp.float32)
        intersection = jnp.zeros((TM_DEV, TN_DEV), jnp.float32)
        for step_index in range(SECTIONS):
            section = sections[step_index].astype(jnp.int32)
            a_panel = lax.dynamic_slice(a_matrix, (row_index * TM_DEV * TILE, section * panel_width), (TM_DEV * TILE, panel_width))
            a_panel_flags = lax.dynamic_slice(a_flags, (row_index * TM_DEV, section * KT), (TM_DEV, KT))
            b_panel = lax.dynamic_slice(b_matrix, (section * panel_width, col_index * TN_DEV * TILE), (panel_width, TN_DEV * TILE))
            b_panel_flags = lax.dynamic_slice(b_flags, (section * KT, col_index * TN_DEV), (KT, TN_DEV))
            a_masked = mask_tiles(a_panel, a_panel_flags, TM_DEV, KT)
            b_masked = mask_tiles(b_panel, b_panel_flags, KT, TN_DEV)
            product = product + jnp.dot(a_masked.astype(jnp.float32), b_masked.astype(jnp.float32), precision=lax.Precision.HIGHEST)
            intersection = intersection + jnp.dot(a_panel_flags.astype(jnp.float32), b_panel_flags.astype(jnp.float32), precision=lax.Precision.HIGHEST)
        occupied = (intersection > 0.5).astype(jnp.int32).reshape(-1)
        tiles = to_tiles(product.astype(jnp.bfloat16), TM_DEV, TN_DEV)
        packed_block = from_tiles(compact(tiles, occupied, TM_DEV * TN_DEV), TM_DEV, TN_DEV)
        return packed_block, jnp.sum(occupied).astype(jnp.int32)

    blocks, filled = lax.map(one_block, jnp.arange(N_ROW * N_COL, dtype=jnp.int32))
    offset = (jnp.cumsum(filled) - filled).astype(jnp.int32)
    slot_ids = jnp.arange(TM_DEV * TN_DEV, dtype=jnp.int32)
    places = jnp.where(slot_ids[None, :] < filled[:, None], offset[:, None] + slot_ids[None, :], -1).astype(jnp.int32)
    tile_place = places.reshape(N_ROW, N_COL, TM_DEV, TN_DEV).transpose(0, 2, 1, 3).reshape(N_ROW * TM_DEV, N_COL * TN_DEV)
    packed = blocks.reshape(N_ROW, N_COL, TM_DEV * TILE, TN_DEV * TILE).transpose(0, 2, 1, 3).reshape(N_ROW * TM_DEV * TILE, N_COL * TN_DEV * TILE)
    return packed, tile_place
```

```python
import functools

import jax
import jax.numpy as jnp
from jax import lax
from jax.experimental import pallas as pl
from jax.experimental.pallas import tpu as pltpu
from jax.sharding import PartitionSpec as P

TILE = 128
SECTIONS = 2
MOST = 64
HALF = MOST // 2
SPAN = 2
STEPS = MOST // SPAN
A_SPAN = 4
A_STEPS = HALF // A_SPAN
BLOCK = 512
MESH = pl.DeviceIdType.MESH
ANY = pl.BlockSpec(memory_space=pl.ANY)
SMEM = pl.BlockSpec(memory_space=pltpu.SMEM)
VMEM = pl.BlockSpec(memory_space=pltpu.VMEM)


def tile_at(ref, p, q):
    rows = pl.ds(pl.multiple_of(p * TILE, TILE), TILE)
    cols = pl.ds(q * TILE if isinstance(q, int) else pl.multiple_of(q * TILE, TILE), TILE)
    return ref.at[rows, cols]


def pack_kernel(tile_rows, panel, tile_cols, ratio, sections, a_flags, b_flags, a_vec, b_vec, a, b, a_out, b_out, flags, sem):
    def gather(occupied, src, out, rows, cols, first):
        def lap(p, rank):
            for q in range(cols):
                here = occupied[first + p, q]

                @pl.when(here == 1)
                def _():
                    pltpu.make_async_copy(tile_at(src, first + p, q), out.at[rank], sem).start()

                rank = rank + here
            return rank

        return lax.fori_loop(0, rows, lap, jnp.int32(0))

    total = jnp.int32(0)
    my_row, my_col = lax.axis_index("row"), lax.axis_index("col")
    mine_a = (sections[0] == my_col) | (sections[1] == my_col)
    for s in range(SECTIONS):
        first = lax.rem(sections[s], ratio) * panel
        total += lax.cond(
            sections[s] // ratio == my_row,
            lambda: gather(b_flags, b, b_out.at[s], panel, tile_cols, first),
            lambda: jnp.int32(0),
        )
    total += lax.cond(mine_a, lambda: gather(a_flags, a, a_out, tile_rows, panel, 0), lambda: jnp.int32(0))

    flags[...] = jnp.zeros_like(flags)
    ahead = tile_rows // panel
    for i in range(ahead):
        flags[i, :, 0:panel] = a_vec[i * panel : (i + 1) * panel, :]
    for i in range(ratio):
        flags[ahead + i, :, 0:tile_cols] = b_vec[i * panel : (i + 1) * panel, :]

    @pl.loop(0, total)
    def _(i):
        pltpu.make_async_copy(tile_at(a, 0, 0), a_out.at[0], sem).wait()


def comm_kernel(
    n_row, n_col, tile_rows, panel, tile_cols, ratio,
    sections, own_a, own_b, flags, done, meta,
    every, staged, table, occ, swapped, held, a0, a1, b0, b1, a_full, b_full, acc, stages,
    local, row_send, row_recv, col_send, col_recv,
    up_send, up_recv, down_send, down_recv, core_send, core_recv, stage_send, stage_recv, last_send, last_recv,
):
    my_row, my_col = lax.axis_index("row"), lax.axis_index("col")
    bits = n_col.bit_length() - 1
    ahead = tile_rows // panel
    side = lax.rem(my_col, 2)
    partner = my_col + 1 - 2 * side
    above = jnp.minimum(my_row + 1, n_row - 1)
    below = jnp.maximum(my_row - 1, 0)
    b_parts, a_parts = (b0, b1), (a0, a1)
    tags = [sections[s] for s in range(SECTIONS)]
    owners = [lax.div(tag, ratio) for tag in tags]

    def flip(bit):
        on = lax.rem(lax.div(my_col, 1 << bit), 2)
        return my_col + (1 << bit) - 2 * on * (1 << bit)

    barrier = pltpu.get_barrier_semaphore()
    for k in range(1, n_row):
        pl.semaphore_signal(barrier, inc=1, device_id=(lax.rem(my_row + k, n_row), my_col), device_id_type=MESH)
    for k in range(1, n_col):
        pl.semaphore_signal(barrier, inc=1, device_id=(my_row, lax.rem(my_col + k, n_col)), device_id_type=MESH)
    pl.semaphore_wait(barrier, n_row + n_col - 2)

    def send(src, dst, send_sem, recv_sem, row, col):
        return pltpu.make_async_remote_copy(
            src_ref=src, dst_ref=dst, send_sem=send_sem, recv_sem=recv_sem,
            device_id=(row, col), device_id_type=MESH,
        )

    def along_row(k):
        return send(
            flags, every.at[my_col, my_row], row_send.at[k], row_recv.at[k], lax.rem(my_row + k, n_row), my_col
        )

    def along_col(k):
        return send(
            every.at[my_col], every.at[my_col], col_send.at[k], col_recv.at[k], my_row, lax.rem(my_col + k, n_col)
        )

    def up(s, c, src=None):
        part = pl.ds(c * SPAN, SPAN)
        i = s * STEPS + c
        src = b_parts[s] if src is None else src
        return send(src.at[part], b_parts[s].at[part], up_send.at[i], up_recv.at[i], above, my_col)

    def down(s, c, src=None):
        part = pl.ds(MOST + c * SPAN, SPAN)
        i = s * STEPS + c
        src = b_parts[s].at[part] if src is None else src.at[pl.ds(c * SPAN, SPAN)]
        return send(src, b_parts[s].at[part], down_send.at[i], down_recv.at[i], below, my_col)

    def core_swap():
        return send(
            own_a.at[pl.ds((1 - side) * HALF, HALF)], swapped, core_send, core_recv, my_row, partner
        )

    def stage(bit, j):
        src = held if bit == 1 else stages.at[bit - 2]
        part = pl.ds(j * A_SPAN, A_SPAN)
        return send(
            src.at[part], stages.at[bit - 1, part], stage_send.at[bit - 1, j], stage_recv.at[bit - 1, j],
            my_row, flip(bit),
        )

    def last(s, j):
        part = pl.ds(side * HALF + j * A_SPAN, A_SPAN)
        i = s * A_STEPS + j
        return send(a_parts[s].at[part], a_parts[s].at[part], last_send.at[i], last_recv.at[i], my_row, partner)

    own = pltpu.make_async_copy(flags, every.at[my_col, my_row], local)
    own.start()
    for k in range(1, n_row):
        along_row(k).start()
    core_swap().start()

    @pl.when(my_row == 0)
    def _():
        for s in range(SECTIONS):

            @pl.loop(0, STEPS)
            def _(c):
                up(s, c, own_b.at[s]).start()

    @pl.when(my_row == n_row - 1)
    def _():
        for s in range(SECTIONS):

            @pl.loop(0, STEPS)
            def _(c):
                down(s, c, own_b.at[s]).start()

    own.wait()
    for k in range(1, n_row):
        along_row(k).wait_recv()
    for k in range(1, n_col):
        along_col(k).start()

    core_swap().wait_recv()
    for s in range(SECTIONS):
        mine = tags[s] == my_col

        @pl.loop(0, HALF)
        def _(k):
            held[s * HALF + k] = jnp.where(mine, own_a[side * HALF + k], swapped[k])

    @pl.loop(0, SECTIONS * A_STEPS)
    def _(j):
        stage(1, j).start()

    def hop(s, c):
        inject = owners[s] == my_row

        @pl.when(my_row > 0)
        def _():
            up(s, c).wait_recv()
            for k in range(SPAN):
                b_parts[s][c * SPAN + k] = jnp.where(inject, own_b[s, c * SPAN + k], b_parts[s][c * SPAN + k])

            @pl.when(my_row < n_row - 1)
            def _():
                up(s, c).start()

        @pl.when(my_row < n_row - 1)
        def _():
            down(s, c).wait_recv()
            for k in range(SPAN):
                spot = MOST + c * SPAN + k
                b_parts[s][spot] = jnp.where(inject, own_b[s, c * SPAN + k], b_parts[s][spot])

            @pl.when(my_row > 0)
            def _():
                down(s, c).start()

    def pass_a(bit, j):
        stage(bit, j).wait_recv()
        final = bit == bits - 1
        for s in range(SECTIONS):

            @pl.when((j >= s * A_STEPS) & (j < (s + 1) * A_STEPS))
            def _():
                near = lax.div(tags[s], 1 << bit) == lax.div(my_col, 1 << bit)
                for k in range(A_SPAN):
                    i = j * A_SPAN + k
                    before = held[i] if bit == 1 else stages[bit - 2, i]
                    got = jnp.where(near, before, stages[bit - 1, i])
                    if final:
                        a_parts[s][side * HALF + i - s * HALF] = got
                    else:
                        stages[bit - 1, i] = got
                if final:
                    last(s, j - s * A_STEPS).start()

        if not final:
            stage(bit + 1, j).start()

    lag = 4

    def pass_all(i):
        for bit in range(1, bits):
            j2 = i - lag * bit

            @pl.when((j2 >= 0) & (j2 < 2 * SECTIONS * A_STEPS) & (lax.rem(j2, 2) == 0))
            def _():
                pass_a(bit, lax.div(j2, 2))

    def step(i, s):
        hop(s, i - s * STEPS)
        pass_all(i)

    first = 4

    @pl.loop(0, first)
    def _(i):
        step(i, 0)

    for k in range(1, n_col):
        along_col(k).wait_recv()

    for s in range(SECTIONS):
        for i in range(ahead):
            staged[s, i] = every[tags[s], my_row, i]
        staged[s, ahead] = every[my_col, owners[s], ahead + lax.rem(tags[s], ratio)]
    tables = pltpu.make_async_copy(staged, table, local)
    tables.start()

    sides = []
    for s in range(SECTIONS):
        rows = [every[tags[s], r, i] for r in range(n_row) for i in range(ahead)]
        sides.append(jnp.concatenate(rows, axis=0).astype(jnp.float32)[:, 0:panel])
    blocks = lax.broadcasted_iota(jnp.int32, (n_row * tile_rows, TILE), 0) // tile_rows * n_col
    me = my_row * n_col + my_col
    lower = jnp.zeros((n_row * tile_rows, TILE), jnp.float32)
    chosen = jnp.zeros((n_row * tile_rows, TILE), jnp.float32)
    for c in range(n_col):
        common = jnp.zeros((n_row * tile_rows, TILE), jnp.float32)
        for s in range(SECTIONS):
            tile_flags = every[c, owners[s], ahead + lax.rem(tags[s], ratio)].astype(jnp.float32)
            common += jnp.dot(sides[s], tile_flags, preferred_element_type=jnp.float32)
        occupied = jnp.where(common > 0.5, 1.0, 0.0)
        lower += jnp.where(blocks + c < me, occupied, 0.0)
        chosen += jnp.where(my_col == c, occupied, 0.0)
    occ[...] = chosen
    offset = jnp.sum(jnp.sum(lower, axis=1, keepdims=True), axis=0, keepdims=True)
    meta[0:tile_rows] = occ[pl.ds(pl.multiple_of(my_row * tile_rows, tile_rows), tile_rows)].astype(jnp.int32)
    meta[tile_rows:] = jnp.broadcast_to(offset, (8, TILE)).astype(jnp.int32)
    tables.wait()

    @pl.loop(first, STEPS)
    def _(i):
        step(i, 0)

    def put(ref, p, cols, rank, flag_at, part, base):
        for q in range(cols):
            here = flag_at(q)
            spot = tile_at(ref, p, q)
            got = part[base + jnp.minimum(rank, MOST - 1)]
            spot[...] = jnp.where(here == 1, got, jnp.zeros_like(got))
            rank = rank + here
        return rank

    def spread_a(s, p, rank):
        return put(a_full, p, panel, rank, lambda q: table[s, lax.div(p, panel), lax.rem(p, panel), q], a_parts[s], 0)

    def spread_b(s, p, rank):
        base = jnp.where((owners[s] >= my_row) & (my_row < n_row - 1), MOST, 0)
        return put(b_full, p, tile_cols, rank, lambda q: table[s, ahead, p, q], b_parts[s], base)

    for j in range(A_STEPS):
        last(0, j).wait_recv()

    def fill_first(c, ranks):
        rank_a, rank_b = ranks
        step(STEPS + c, 1)
        for k in range(tile_rows // panel):
            rank_a = spread_a(0, c * (tile_rows // panel) + k, rank_a)
        rank_b = spread_b(0, c, rank_b)
        return rank_a, rank_b

    lax.fori_loop(0, panel, fill_first, (jnp.int32(0), jnp.int32(0)))

    across = tile_cols * TILE // BLOCK
    down_blocks = tile_rows * TILE // BLOCK

    def block_of(j):
        rows = pl.ds(pl.multiple_of(lax.div(j, across) * BLOCK, BLOCK), BLOCK)
        cols = pl.ds(pl.multiple_of(lax.rem(j, across) * BLOCK, BLOCK), BLOCK)
        return rows, cols

    def product(j):
        rows, cols = block_of(j)
        return rows, cols, jnp.dot(a_full[rows, :], b_full[:, cols], preferred_element_type=jnp.float32)

    pieces = across * down_blocks

    @pl.loop(0, pieces)
    def _(j):
        step(STEPS + panel + j, 1)
        rows, cols, got = product(j)
        acc[rows, cols] = got

    @pl.loop(panel + pieces, STEPS - panel)
    def _(c):
        step(STEPS + c, 1)

    for j in range(A_STEPS):
        last(1, j).wait_recv()

    def fill_second(c, rank_a):
        step(2 * STEPS - panel + c, 1)
        for k in range(tile_rows // panel):
            rank_a = spread_a(1, c * (tile_rows // panel) + k, rank_a)
        return rank_a

    lax.fori_loop(0, panel, fill_second, jnp.int32(0))
    lax.fori_loop(0, panel, functools.partial(spread_b, 1), jnp.int32(0))

    @pl.loop(0, pieces)
    def _(j):
        rows, cols, got = product(j)
        done[rows, cols] = (acc[rows, cols] + got).astype(done.dtype)

    for k in range(1, n_row):
        along_row(k).wait_send()
    for k in range(1, n_col):
        along_col(k).wait_send()
    core_swap().wait_send()
    for s in range(SECTIONS):

        @pl.loop(0, A_STEPS)
        def _(j):
            last(s, j).wait_send()

        @pl.loop(0, STEPS)
        def _(c):
            @pl.when(my_row < n_row - 1)
            def _():
                up(s, c).wait_send()

            @pl.when(my_row > 0)
            def _():
                down(s, c).wait_send()

    for bit in range(1, bits):

        @pl.loop(0, SECTIONS * A_STEPS)
        def _(j):
            stage(bit, j).wait_send()


def final_kernel(tile_rows, tile_cols, meta, done, out, places, zero, sem):
    zero[...] = jnp.zeros_like(zero)

    def lap(p, rank):
        for q in range(tile_cols):
            here = meta[p, q]

            @pl.when(here == 1)
            def _():
                spot = tile_at(out, lax.div(rank, tile_cols), lax.rem(rank, tile_cols))
                pltpu.make_async_copy(tile_at(done, p, q), spot, sem).start()

            rank = rank + here
        return rank

    filled = lax.fori_loop(0, tile_rows, lap, jnp.int32(0))

    @pl.loop(filled, tile_rows * tile_cols)
    def _(k):
        pltpu.make_async_copy(zero, tile_at(out, lax.div(k, tile_cols), lax.rem(k, tile_cols)), sem).start()

    slot = lax.broadcasted_iota(jnp.int32, places.shape, 0) * tile_cols + lax.broadcasted_iota(jnp.int32, places.shape, 1)
    places[...] = jnp.where(slot < filled, meta[tile_rows, 0] + slot, -1)
    pltpu.make_async_copy(done, out, sem).wait()


def shards(n_row, n_col, a_matrix, a_flags, b_matrix, b_flags, sections):
    tile_rows, panel = a_flags.shape
    tile_cols = b_flags.shape[1]
    ratio = n_col // n_row
    dtype = a_matrix.dtype
    bits = n_col.bit_length() - 1
    ahead = tile_rows // panel

    def tiles(*lead):
        return lead + (TILE, TILE)

    own_a, own_b, flags = pl.pallas_call(
        functools.partial(pack_kernel, tile_rows, panel, tile_cols, ratio),
        out_shape=(
            jax.ShapeDtypeStruct(tiles(MOST), dtype),
            jax.ShapeDtypeStruct(tiles(SECTIONS, MOST), dtype),
            jax.ShapeDtypeStruct((ahead + ratio, panel, TILE), jnp.int32),
        ),
        in_specs=[SMEM, SMEM, SMEM, VMEM, VMEM, ANY, ANY],
        out_specs=(VMEM, VMEM, VMEM),
        scratch_shapes=[pltpu.SemaphoreType.DMA],
        compiler_params=pltpu.CompilerParams(vmem_limit_bytes=16 * 1024 * 1024),
        name="pack",
    )(sections, a_flags, b_flags, a_flags, b_flags, a_matrix, b_matrix)

    size = (tile_rows * TILE, tile_cols * TILE)
    dma = pltpu.SemaphoreType.DMA
    done, meta = pl.pallas_call(
        functools.partial(comm_kernel, n_row, n_col, tile_rows, panel, tile_cols, ratio),
        out_shape=(jax.ShapeDtypeStruct(size, dtype), jax.ShapeDtypeStruct((tile_rows + 8, TILE), jnp.int32)),
        in_specs=[SMEM, VMEM, VMEM, VMEM],
        out_specs=(VMEM, VMEM),
        scratch_shapes=[
            pltpu.VMEM((n_col, n_row, ahead + ratio, panel, TILE), jnp.int32),
            pltpu.VMEM((SECTIONS, ahead + 1, panel, TILE), jnp.int32),
            pltpu.SMEM((SECTIONS, ahead + 1, panel, TILE), jnp.int32),
            pltpu.VMEM((n_row * tile_rows, TILE), jnp.float32),
            pltpu.VMEM(tiles(HALF), dtype),
            pltpu.VMEM(tiles(MOST), dtype),
            pltpu.VMEM(tiles(MOST), dtype),
            pltpu.VMEM(tiles(MOST), dtype),
            pltpu.VMEM(tiles(2 * MOST), dtype),
            pltpu.VMEM(tiles(2 * MOST), dtype),
            pltpu.VMEM((tile_rows * TILE, panel * TILE), dtype),
            pltpu.VMEM((panel * TILE, tile_cols * TILE), dtype),
            pltpu.VMEM(size, jnp.float32),
            pltpu.VMEM(tiles(bits - 1, MOST), dtype),
            dma, dma((n_row,)), dma((n_row,)), dma((n_col,)), dma((n_col,)),
            dma((SECTIONS * STEPS,)), dma((SECTIONS * STEPS,)), dma((SECTIONS * STEPS,)), dma((SECTIONS * STEPS,)),
            dma, dma,
            dma((bits - 1, SECTIONS * A_STEPS)), dma((bits - 1, SECTIONS * A_STEPS)),
            dma((SECTIONS * A_STEPS,)), dma((SECTIONS * A_STEPS,)),
        ],
        compiler_params=pltpu.CompilerParams(
            collective_id=0, has_side_effects=True, vmem_limit_bytes=67043328
        ),
        name="exchange",
    )(sections, own_a, own_b, flags)

    return pl.pallas_call(
        functools.partial(final_kernel, tile_rows, tile_cols),
        out_shape=(jax.ShapeDtypeStruct(size, dtype), jax.ShapeDtypeStruct((tile_rows, tile_cols), jnp.int32)),
        in_specs=[SMEM, VMEM],
        out_specs=(ANY, VMEM),
        scratch_shapes=[pltpu.VMEM((TILE, TILE), dtype), pltpu.SemaphoreType.DMA],
        compiler_params=pltpu.CompilerParams(vmem_limit_bytes=16 * 1024 * 1024),
        name="compact",
    )(meta, done)


def solution(mesh):
    return jax.shard_map(
        functools.partial(shards, mesh.shape["row"], mesh.shape["col"]),
        mesh=mesh,
        in_specs=(P("row", "col"), P("row", "col"), P("row", "col"), P("row", "col"), P()),
        out_specs=(P("row", "col"), P("row", "col")),
        check_vma=False,
    )
```

```python
import functools

import jax
import jax.numpy as jnp
from jax import lax
from jax.experimental import pallas as pl
from jax.experimental.pallas import tpu as pltpu
from jax.sharding import PartitionSpec as P

TILE = 128
SECTIONS = 2
MOST = 64
HALF = MOST // 2
SPAN = 2
STEPS = MOST // SPAN
A_SPAN = 4
A_STEPS = HALF // A_SPAN
BLOCK = 512
WINDOW = 6
SKEW = 3
MESH = pl.DeviceIdType.MESH
HBM = pl.BlockSpec(memory_space=pltpu.HBM)
SMEM = pl.BlockSpec(memory_space=pltpu.SMEM)
VMEM = pl.BlockSpec(memory_space=pltpu.VMEM)


def tile_at(ref, p, q):
    rows = pl.ds(pl.multiple_of(p * TILE, TILE), TILE)
    cols = pl.ds(q * TILE if isinstance(q, int) else pl.multiple_of(q * TILE, TILE), TILE)
    return ref.at[rows, cols]


def block_at(j):
    return pl.ds(pl.multiple_of(j * BLOCK, BLOCK), BLOCK)


def pack_kernel(
    tile_rows, panel, tile_cols, ratio, sections_in, a_flags_in, b_flags_in, a, b,
    a_out, b_out, flags, sections, a_flags, b_flags, a_vec, b_vec, sems, sem,
):
    moves = (
        (sections_in, sections), (b_flags_in, b_flags), (a_flags_in, a_flags), (a_flags_in, a_vec), (b_flags_in, b_vec)
    )
    loads = [pltpu.make_async_copy(src, dst, sems.at[i]) for i, (src, dst) in enumerate(moves)]
    for load in loads:
        load.start()
    flags[...] = jnp.zeros_like(flags)
    for load in loads:
        load.wait()

    def gather(occupied, src, out, rows, cols, first, turned):
        def lap(p, rank):
            for q in range(cols):
                here = occupied[q, p] if turned else occupied[first + p, q]

                @pl.when(here == 1)
                def _():
                    pltpu.make_async_copy(tile_at(src, first + p, q), out.at[rank], sem).start()

                rank = rank + here
            return rank

        return lax.fori_loop(0, rows, lap, jnp.int32(0))

    total = jnp.int32(0)
    my_row, my_col = lax.axis_index("row"), lax.axis_index("col")
    mine_a = (sections[0] == my_col) | (sections[1] == my_col)
    for s in range(SECTIONS):
        first = lax.rem(sections[s], ratio) * panel
        total += lax.cond(
            sections[s] // ratio == my_row,
            lambda: gather(b_flags, b, b_out.at[s], panel, tile_cols, first, False),
            lambda: jnp.int32(0),
        )
    total += lax.cond(mine_a, lambda: gather(a_flags, a, a_out, tile_rows, panel, 0, True), lambda: jnp.int32(0))

    flags[0, :, 0:tile_rows] = a_vec[...]
    for i in range(ratio):
        flags[1 + i, :, 0:tile_cols] = b_vec[i * panel : (i + 1) * panel, :]

    @pl.loop(0, total)
    def _(i):
        pltpu.make_async_copy(tile_at(a, 0, 0), a_out.at[0], sem).wait()


def comm_kernel(
    n_row, n_col, tile_rows, panel, tile_cols, ratio,
    sections_in, own_a, own_b, flags, acc0, acc1, a_full, b_full, meta,
    sections, every, staged, table, occ, swapped, held, a0, a1, b0, b1, stages,
    local, brief, row_send, row_recv, col_send, col_recv,
    up_send, up_recv, down_send, down_recv, core_send, core_recv, stage_send, stage_recv, last_send, last_recv,
):
    my_row, my_col = lax.axis_index("row"), lax.axis_index("col")
    bits = n_col.bit_length() - 1
    side = lax.rem(my_col, 2)
    partner = my_col + 1 - 2 * side
    above = jnp.minimum(my_row + 1, n_row - 1)
    below = jnp.maximum(my_row - 1, 0)
    b_parts, a_parts = (b0, b1), (a0, a1)

    def flip(bit):
        on = lax.rem(lax.div(my_col, 1 << bit), 2)
        return my_col + (1 << bit) - 2 * on * (1 << bit)

    choice = pltpu.make_async_copy(sections_in, sections, brief)
    choice.start()
    barrier = pltpu.get_barrier_semaphore()
    for k in range(1, n_row):
        pl.semaphore_signal(barrier, inc=1, device_id=(lax.rem(my_row + k, n_row), my_col), device_id_type=MESH)
    for k in range(1, n_col):
        pl.semaphore_signal(barrier, inc=1, device_id=(my_row, lax.rem(my_col + k, n_col)), device_id_type=MESH)
    pl.semaphore_wait(barrier, n_row + n_col - 2)

    def send(src, dst, send_sem, recv_sem, row, col):
        return pltpu.make_async_remote_copy(
            src_ref=src, dst_ref=dst, send_sem=send_sem, recv_sem=recv_sem,
            device_id=(row, col), device_id_type=MESH,
        )

    def along_row(k):
        return send(
            flags, every.at[my_col, my_row], row_send.at[k], row_recv.at[k], lax.rem(my_row + k, n_row), my_col
        )

    def along_col(k):
        return send(
            every.at[my_col], every.at[my_col], col_send.at[k], col_recv.at[k], my_row, lax.rem(my_col + k, n_col)
        )

    def up(s, c, src=None):
        part = pl.ds(c * SPAN, SPAN)
        i = s * STEPS + c
        src = b_parts[s] if src is None else src
        return send(src.at[part], b_parts[s].at[part], up_send.at[i], up_recv.at[i], above, my_col)

    def down(s, c, src=None):
        part = pl.ds(MOST + c * SPAN, SPAN)
        i = s * STEPS + c
        src = b_parts[s].at[part] if src is None else src.at[pl.ds(c * SPAN, SPAN)]
        return send(src, b_parts[s].at[part], down_send.at[i], down_recv.at[i], below, my_col)

    def core_swap():
        return send(
            own_a.at[pl.ds((1 - side) * HALF, HALF)], swapped, core_send, core_recv, my_row, partner
        )

    def stage(bit, j):
        src = held if bit == 1 else stages.at[bit - 2]
        part = pl.ds(j * A_SPAN, A_SPAN)
        return send(
            src.at[part], stages.at[bit - 1, part], stage_send.at[bit - 1, j], stage_recv.at[bit - 1, j],
            my_row, flip(bit),
        )

    def last(s, j):
        part = pl.ds(side * HALF + j * A_SPAN, A_SPAN)
        i = s * A_STEPS + j
        return send(a_parts[s].at[part], a_parts[s].at[part], last_send.at[i], last_recv.at[i], my_row, partner)

    own = pltpu.make_async_copy(flags, every.at[my_col, my_row], local)
    own.start()
    for k in range(1, n_row):
        along_row(k).start()
    core_swap().start()

    @pl.when(my_row == 0)
    def _():
        @pl.loop(0, WINDOW)
        def _(c):
            up(0, c, own_b.at[0]).start()

    @pl.when(my_row == n_row - 1)
    def _():
        @pl.loop(0, WINDOW)
        def _(c):
            down(0, c, own_b.at[0]).start()

    own.wait()
    for k in range(1, n_row):
        along_row(k).wait_recv()
    for k in range(1, n_col):
        along_col(k).start()

    choice.wait()
    tags = [sections[s] for s in range(SECTIONS)]
    owners = [lax.div(tag, ratio) for tag in tags]
    core_swap().wait_recv()
    for s in range(SECTIONS):
        mine = tags[s] == my_col

        @pl.loop(0, HALF)
        def _(k):
            held[s * HALF + k] = jnp.where(mine, own_a[side * HALF + k], swapped[k])

    @pl.loop(0, SECTIONS * A_STEPS)
    def _(j):
        stage(1, j).start()

    def parted(g, body):
        for s in range(SECTIONS):

            @pl.when((g >= s * STEPS) & (g < (s + 1) * STEPS))
            def _():
                body(s, g - s * STEPS)

    def feed(way, i):
        parted(i, lambda s, c: way(s, c).wait_send())
        parted(i + WINDOW, lambda s, c: way(s, c, own_b.at[s]).start())

    def take(way, first, onward, s, c):
        way(s, c).wait_recv()
        inject = owners[s] == my_row
        for k in range(SPAN):
            spot = first + c * SPAN + k
            b_parts[s][spot] = jnp.where(inject, own_b[s, c * SPAN + k], b_parts[s][spot])

        @pl.when(onward)
        def _():
            way(s, c).start()

    def hop(i):
        @pl.when(my_row == 0)
        def _():
            feed(up, i)

        @pl.when(my_row == n_row - 1)
        def _():
            feed(down, i)

        @pl.when(my_row > 0)
        def _():
            parted(i - SKEW * my_row, functools.partial(take, up, 0, my_row < n_row - 1))

        @pl.when(my_row < n_row - 1)
        def _():
            parted(i - SKEW * (n_row - 1 - my_row), functools.partial(take, down, MOST, my_row > 0))

    def pass_a(bit, j):
        stage(bit, j).wait_recv()
        final = bit == bits - 1
        for s in range(SECTIONS):

            @pl.when((j >= s * A_STEPS) & (j < (s + 1) * A_STEPS))
            def _():
                near = lax.div(tags[s], 1 << bit) == lax.div(my_col, 1 << bit)
                for k in range(A_SPAN):
                    i = j * A_SPAN + k
                    before = held[i] if bit == 1 else stages[bit - 2, i]
                    got = jnp.where(near, before, stages[bit - 1, i])
                    if final:
                        a_parts[s][side * HALF + i - s * HALF] = got
                    else:
                        stages[bit - 1, i] = got
                if final:
                    last(s, j - s * A_STEPS).start()

        if not final:
            stage(bit + 1, j).start()

    lag = 4

    def pass_all(i):
        for bit in range(1, bits):
            j2 = i - lag * bit

            @pl.when((j2 >= 0) & (j2 < 2 * SECTIONS * A_STEPS) & (lax.rem(j2, 2) == 0))
            def _():
                pass_a(bit, lax.div(j2, 2))

    def step(i):
        hop(i)
        pass_all(i)

    start = STEPS + SKEW * (n_row - 1)

    first = 4

    @pl.loop(0, first)
    def _(i):
        step(i)

    for k in range(1, n_col):
        along_col(k).wait_recv()

    for s in range(SECTIONS):
        staged[s, 0] = every[tags[s], my_row, 0]
        staged[s, 1] = every[my_col, owners[s], 1 + lax.rem(tags[s], ratio)]
    tables = pltpu.make_async_copy(staged, table, local)
    tables.start()

    sides = []
    for s in range(SECTIONS):
        rows = [every[tags[s], r, 0].astype(jnp.float32).T[0:tile_rows] for r in range(n_row)]
        sides.append(jnp.concatenate(rows, axis=0))
    blocks = lax.broadcasted_iota(jnp.int32, (n_row * tile_rows, TILE), 0) // tile_rows * n_col
    me = my_row * n_col + my_col
    lower = jnp.zeros((n_row * tile_rows, TILE), jnp.float32)
    chosen = jnp.zeros((n_row * tile_rows, TILE), jnp.float32)
    for c in range(n_col):
        common = jnp.zeros((n_row * tile_rows, TILE), jnp.float32)
        for s in range(SECTIONS):
            tile_flags = every[c, owners[s], 1 + lax.rem(tags[s], ratio)].astype(jnp.float32)
            common += jnp.dot(sides[s], tile_flags, preferred_element_type=jnp.float32)
        occupied = jnp.where(common > 0.5, 1.0, 0.0)
        lower += jnp.where(blocks + c < me, occupied, 0.0)
        chosen += jnp.where(my_col == c, occupied, 0.0)
    occ[...] = chosen
    offset = jnp.sum(jnp.sum(lower, axis=1, keepdims=True), axis=0, keepdims=True)
    meta[0:tile_rows] = occ[pl.ds(pl.multiple_of(my_row * tile_rows, tile_rows), tile_rows)].astype(jnp.int32)
    meta[tile_rows:] = jnp.broadcast_to(offset, (8, TILE)).astype(jnp.int32)
    tables.wait()

    @pl.loop(first, start)
    def _(i):
        step(i)

    def put(ref, p, cols, rank, flag_at, part, base):
        for q in range(cols):
            here = flag_at(q)
            spot = tile_at(ref, p, q)
            got = part[base + jnp.minimum(rank, MOST - 1)]
            spot[...] = jnp.where(here == 1, got, jnp.zeros_like(got))
            rank = rank + here
        return rank

    def spread_a(s, p, rank):
        return put(a_full, p, panel, rank, lambda q: table[s, 0, q, p], a_parts[s], 0)

    def spread_b(s, p, rank):
        base = jnp.where((owners[s] >= my_row) & (my_row < n_row - 1), MOST, 0)
        return put(b_full, p, tile_cols, rank, lambda q: table[s, 1, p, q], b_parts[s], base)

    for j in range(A_STEPS):
        last(0, j).wait_recv()

    def fill_first(c, ranks):
        rank_a, rank_b = ranks
        step(start + c)
        for k in range(tile_rows // panel):
            rank_a = spread_a(0, c * (tile_rows // panel) + k, rank_a)
        rank_b = spread_b(0, c, rank_b)
        return rank_a, rank_b

    lax.fori_loop(0, panel, fill_first, (jnp.int32(0), jnp.int32(0)))

    across = tile_cols * TILE // BLOCK
    down_blocks = tile_rows * TILE // BLOCK
    pieces = across * down_blocks

    for h, acc in enumerate((acc0, acc1)):

        @pl.loop(0, pieces // 2)
        def _(j):
            step(start + panel + h * (pieces // 2) + j)
            i = lax.div(j, across)
            rows, cols = block_at(h * (down_blocks // 2) + i), block_at(lax.rem(j, across))
            acc[block_at(i), cols] = jnp.dot(a_full[rows, :], b_full[:, cols], preferred_element_type=jnp.float32)

    @pl.loop(panel + pieces, STEPS - panel)
    def _(c):
        step(start + c)

    for j in range(A_STEPS):
        last(1, j).wait_recv()

    def fill_second(c, rank_a):
        step(start + STEPS - panel + c)
        for k in range(tile_rows // panel):
            rank_a = spread_a(1, c * (tile_rows // panel) + k, rank_a)
        return rank_a

    lax.fori_loop(0, panel, fill_second, jnp.int32(0))
    lax.fori_loop(0, panel, functools.partial(spread_b, 1), jnp.int32(0))

    for k in range(1, n_row):
        along_row(k).wait_send()
    for k in range(1, n_col):
        along_col(k).wait_send()
    core_swap().wait_send()
    for s in range(SECTIONS):

        @pl.loop(0, A_STEPS)
        def _(j):
            last(s, j).wait_send()

        @pl.loop(0, STEPS)
        def _(c):
            @pl.when((my_row > 0) & (my_row < n_row - 1))
            def _():
                up(s, c).wait_send()
                down(s, c).wait_send()

    for bit in range(1, bits):

        @pl.loop(0, SECTIONS * A_STEPS)
        def _(j):
            stage(bit, j).wait_send()


def final_kernel(tile_rows, tile_cols, meta_in, acc0, acc1, a_full, b_full, out, places, meta, done, zero, local, sem):
    load = pltpu.make_async_copy(meta_in, meta, local)
    load.start()
    zero[...] = jnp.zeros_like(zero)
    across = tile_cols * TILE // BLOCK
    down = tile_rows * TILE // BLOCK
    span = BLOCK // TILE
    load.wait()

    def slab(h, acc, i, rank):
        rows = block_at(h * (down // 2) + i)

        @pl.loop(0, across)
        def _(j):
            cols = block_at(j)
            got = jnp.dot(a_full[rows, :], b_full[:, cols], preferred_element_type=jnp.float32)
            done[rows, cols] = (acc[block_at(i), cols] + got).astype(done.dtype)

        def lap(r, rank):
            p = (h * (down // 2) + i) * span + r
            for q in range(tile_cols):
                here = meta[p, q]

                @pl.when(here == 1)
                def _():
                    spot = tile_at(out, lax.div(rank, tile_cols), lax.rem(rank, tile_cols))
                    pltpu.make_async_copy(tile_at(done, p, q), spot, sem).start()

                rank = rank + here
            return rank

        return lax.fori_loop(0, span, lap, rank)

    filled = jnp.int32(0)
    for h, acc in enumerate((acc0, acc1)):
        filled = lax.fori_loop(0, down // 2, functools.partial(slab, h, acc), filled)

    @pl.loop(filled, tile_rows * tile_cols)
    def _(k):
        pltpu.make_async_copy(zero, tile_at(out, lax.div(k, tile_cols), lax.rem(k, tile_cols)), sem).start()

    down_slots = lax.broadcasted_iota(jnp.int32, places.shape, 0) * tile_cols
    slot = down_slots + lax.broadcasted_iota(jnp.int32, places.shape, 1)
    places[...] = jnp.where(slot < filled, meta[tile_rows, 0] + slot, -1)
    pltpu.make_async_copy(done, out, sem).wait()


def in_hbm(x):
    return pltpu.with_memory_space_constraint(x, pltpu.HBM)


def in_vmem(x):
    return pltpu.with_memory_space_constraint(x, pltpu.VMEM)


def shards(n_row, n_col, a_matrix, a_flags, b_matrix, b_flags, sections):
    tile_rows, panel = a_flags.shape
    tile_cols = b_flags.shape[1]
    ratio = n_col // n_row
    dtype = a_matrix.dtype
    bits = n_col.bit_length() - 1
    dma = pltpu.SemaphoreType.DMA

    def tiles(*lead):
        return lead + (TILE, TILE)

    own_a, own_b, flags = pl.pallas_call(
        functools.partial(pack_kernel, tile_rows, panel, tile_cols, ratio),
        out_shape=(
            pltpu.VMEM(tiles(MOST), dtype),
            pltpu.VMEM(tiles(SECTIONS, MOST), dtype),
            pltpu.VMEM((1 + ratio, panel, TILE), jnp.int32),
        ),
        in_specs=[HBM] * 5,
        out_specs=(VMEM, VMEM, VMEM),
        scratch_shapes=[
            pltpu.SMEM((SECTIONS,), jnp.int32),
            pltpu.SMEM((panel, tile_rows), jnp.int32),
            pltpu.SMEM(b_flags.shape, jnp.int32),
            pltpu.VMEM((panel, tile_rows), jnp.int32),
            pltpu.VMEM(b_flags.shape, jnp.int32),
            dma((5,)), dma,
        ],
        compiler_params=pltpu.CompilerParams(vmem_limit_bytes=16 * 1024 * 1024),
        name="pack",
    )(*[in_hbm(x) for x in (sections, a_flags.T, b_flags, a_matrix, b_matrix)])

    size = (tile_rows * TILE, tile_cols * TILE)
    acc0, acc1, a_full, b_full, meta = pl.pallas_call(
        functools.partial(comm_kernel, n_row, n_col, tile_rows, panel, tile_cols, ratio),
        out_shape=(
            pltpu.VMEM((size[0] // 2, size[1]), jnp.float32),
            pltpu.VMEM((size[0] // 2, size[1]), jnp.float32),
            pltpu.VMEM((tile_rows * TILE, panel * TILE), dtype),
            pltpu.VMEM((panel * TILE, tile_cols * TILE), dtype),
            pltpu.VMEM((tile_rows + 8, TILE), jnp.int32),
        ),
        in_specs=[HBM, VMEM, VMEM, VMEM],
        out_specs=(VMEM,) * 5,
        scratch_shapes=[
            pltpu.SMEM((SECTIONS,), jnp.int32),
            pltpu.VMEM((n_col, n_row, 1 + ratio, panel, TILE), jnp.int32),
            pltpu.VMEM((SECTIONS, 2, panel, TILE), jnp.int32),
            pltpu.SMEM((SECTIONS, 2, panel, TILE), jnp.int32),
            pltpu.VMEM((n_row * tile_rows, TILE), jnp.float32),
            pltpu.VMEM(tiles(HALF), dtype),
            pltpu.VMEM(tiles(MOST), dtype),
            pltpu.VMEM(tiles(MOST), dtype),
            pltpu.VMEM(tiles(MOST), dtype),
            pltpu.VMEM(tiles(2 * MOST), dtype),
            pltpu.VMEM(tiles(2 * MOST), dtype),
            pltpu.VMEM(tiles(bits - 1, MOST), dtype),
            dma, dma, dma((n_row,)), dma((n_row,)), dma((n_col,)), dma((n_col,)),
            dma((SECTIONS * STEPS,)), dma((SECTIONS * STEPS,)), dma((SECTIONS * STEPS,)), dma((SECTIONS * STEPS,)),
            dma, dma,
            dma((bits - 1, SECTIONS * A_STEPS)), dma((bits - 1, SECTIONS * A_STEPS)),
            dma((SECTIONS * A_STEPS,)), dma((SECTIONS * A_STEPS,)),
        ],
        compiler_params=pltpu.CompilerParams(
            collective_id=0, has_side_effects=True, vmem_limit_bytes=24 * 1024 * 1024
        ),
        name="exchange",
    )(in_hbm(sections), *[in_vmem(x) for x in (own_a, own_b, flags)])

    return pl.pallas_call(
        functools.partial(final_kernel, tile_rows, tile_cols),
        out_shape=(jax.ShapeDtypeStruct(size, dtype), jax.ShapeDtypeStruct((tile_rows, tile_cols), jnp.int32)),
        in_specs=[VMEM] * 5,
        out_specs=(HBM, VMEM),
        scratch_shapes=[
            pltpu.SMEM(meta.shape, jnp.int32), pltpu.VMEM(size, dtype), pltpu.VMEM((TILE, TILE), dtype), dma, dma
        ],
        compiler_params=pltpu.CompilerParams(vmem_limit_bytes=12 * 1024 * 1024),
        name="compact",
    )(*[in_vmem(x) for x in (meta, acc0, acc1, a_full, b_full)])


def solution(mesh):
    return jax.shard_map(
        functools.partial(shards, mesh.shape["row"], mesh.shape["col"]),
        mesh=mesh,
        in_specs=(P("row", "col"), P("row", "col"), P("row", "col"), P("row", "col"), P()),
        out_specs=(P("row", "col"), P("row", "col")),
        check_vma=False,
    )
```

```python
import functools

import jax
import jax.numpy as jnp
from jax import lax
from jax.experimental import pallas as pl
from jax.experimental.pallas import tpu as pltpu
from jax.sharding import PartitionSpec as P

TILE = 128
SECTIONS = 2
MOST = 64
HALF = MOST // 2
SPAN = 2
LOW = MOST // SPAN
LENGTHS = (64, 80, 88, 96, 104, 112, 128)
A_SPAN = 4
A_STEPS = HALF // A_SPAN
BLOCK = 512
SKEW = 3
MESH = pl.DeviceIdType.MESH
HBM = pl.BlockSpec(memory_space=pltpu.HBM)
SMEM = pl.BlockSpec(memory_space=pltpu.SMEM)
VMEM = pl.BlockSpec(memory_space=pltpu.VMEM)


def tile_at(ref, p, q):
    rows = pl.ds(pl.multiple_of(p * TILE, TILE), TILE)
    cols = pl.ds(q * TILE if isinstance(q, int) else pl.multiple_of(q * TILE, TILE), TILE)
    return ref.at[rows, cols]


def block_at(j, size=BLOCK):
    return pl.ds(pl.multiple_of(j * size, size), size)


def pack_kernel(
    tile_rows, panel, tile_cols, ratio, sections_in, a_flags_in, b_flags_in, a, b,
    a_out, b_out, flags, sections, a_flags, b_flags, a_vec, b_vec, sems, sem,
):
    moves = (
        (sections_in, sections), (b_flags_in, b_flags), (a_flags_in, a_flags), (a_flags_in, a_vec), (b_flags_in, b_vec)
    )
    loads = [pltpu.make_async_copy(src, dst, sems.at[i]) for i, (src, dst) in enumerate(moves)]
    for load in loads:
        load.start()
    flags[...] = jnp.zeros_like(flags)
    for load in loads:
        load.wait()

    def gather(occupied, src, out, base, rows, cols, first, turned):
        def lap(p, rank):
            for q in range(cols):
                here = occupied[q, p] if turned else occupied[first + p, q]

                @pl.when(here == 1)
                def _():
                    pltpu.make_async_copy(tile_at(src, first + p, q), out.at[base + rank], sem).start()

                rank = rank + here
            return rank

        return lax.fori_loop(0, rows, lap, jnp.int32(0))

    total = jnp.int32(0)
    my_row, my_col = lax.axis_index("row"), lax.axis_index("col")
    mine_a = (sections[0] == my_col) | (sections[1] == my_col)
    for s in range(SECTIONS):
        first = lax.rem(sections[s], ratio) * panel
        total += lax.cond(
            sections[s] // ratio == my_row,
            lambda: gather(b_flags, b, b_out, s * MOST, panel, tile_cols, first, False),
            lambda: jnp.int32(0),
        )
    total += lax.cond(mine_a, lambda: gather(a_flags, a, a_out, 0, tile_rows, panel, 0, True), lambda: jnp.int32(0))

    flags[0, :, 0:tile_rows] = a_vec[...]
    for i in range(ratio):
        flags[1 + i, :, 0:tile_cols] = b_vec[i * panel : (i + 1) * panel, :]

    @pl.loop(0, total)
    def _(i):
        pltpu.make_async_copy(tile_at(a, 0, 0), a_out.at[0], sem).wait()


def count_kernel(
    n_row, n_col, ratio, sections_in, b_flags, sums, pick,
    counts, b_vec, every, sections, local, brief, row_send, row_recv, col_send, col_recv,
):
    my_row, my_col = lax.axis_index("row"), lax.axis_index("col")
    choice = pltpu.make_async_copy(sections_in, sections, brief)
    load = pltpu.make_async_copy(b_flags, b_vec, local)
    choice.start()
    load.start()
    greet(n_row, n_col, my_row, my_col)
    choice.wait()
    load.wait()
    for s in range(SECTIONS):
        found = b_vec[lax.rem(sections[s], ratio)].astype(jnp.float32)
        found = jnp.sum(jnp.sum(found, axis=1, keepdims=True), axis=0, keepdims=True)
        found = jnp.where(lax.div(sections[s], ratio) == my_row, found, jnp.zeros_like(found))
        counts[s : s + 1, :] = jnp.broadcast_to(found, (1, TILE)).astype(jnp.int32)
    along_row, along_col = gathering(
        n_row, n_col, my_row, my_col, counts, every, row_send, row_recv, col_send, col_recv
    )
    for k in range(1, n_row):
        along_row(k).start()
    own = pltpu.make_async_copy(counts, every.at[my_col, my_row], local)
    own.start()
    own.wait()
    for k in range(1, n_row):
        along_row(k).wait_recv()
    for k in range(1, n_col):
        along_col(k).start()
    for k in range(1, n_col):
        along_col(k).wait_recv()

    again = sections[0] == sections[1]
    weight = jnp.where(again, 0, 1)
    most = jnp.zeros((1, TILE), jnp.int32)
    for c in range(0, n_col, 2):
        pair = jnp.zeros((1, TILE), jnp.int32)
        for d in (c, c + 1):
            whole = sum(every[d, r] for r in range(n_row))
            sums[d] = whole
            pair += whole[0:1] + whole[1:2] * weight
        most = jnp.maximum(most, pair)
    level = 1 + sum(jnp.where(most > 2 * length, 1, 0) for length in LENGTHS[1:-1])
    pick[...] = jnp.where(again, 0, level)

    for k in range(1, n_row):
        along_row(k).wait_send()
    for k in range(1, n_col):
        along_col(k).wait_send()


def greet(n_row, n_col, my_row, my_col):
    barrier = pltpu.get_barrier_semaphore()
    for k in range(1, n_row):
        pl.semaphore_signal(barrier, inc=1, device_id=(lax.rem(my_row + k, n_row), my_col), device_id_type=MESH)
    for k in range(1, n_col):
        pl.semaphore_signal(barrier, inc=1, device_id=(my_row, lax.rem(my_col + k, n_col)), device_id_type=MESH)
    pl.semaphore_wait(barrier, n_row + n_col - 2)


def gathering(n_row, n_col, my_row, my_col, mine, every, row_send, row_recv, col_send, col_recv):
    def along_row(k):
        return send(
            mine, every.at[my_col, my_row], row_send.at[k], row_recv.at[k], lax.rem(my_row + k, n_row), my_col
        )

    def along_col(k):
        return send(
            every.at[my_col], every.at[my_col], col_send.at[k], col_recv.at[k], my_row, lax.rem(my_col + k, n_col)
        )

    return along_row, along_col


def send(src, dst, send_sem, recv_sem, row, col):
    return pltpu.make_async_remote_copy(
        src_ref=src, dst_ref=dst, send_sem=send_sem, recv_sem=recv_sem, device_id=(row, col), device_id_type=MESH
    )


def comm_kernel(
    length, n_row, n_col, tile_rows, panel, tile_cols, ratio,
    sections_in, own_a, own_b, flags, sums, done, meta,
    sections, totals, every, staged, table, begin, occ, swapped, held, a0, a1, b_low, b_high, pal, give, got_back, stages,
    acc, a_full, b_full,
    local, brief, tiny, pal_send, pal_recv, row_send, row_recv, col_send, col_recv,
    up_send, up_recv, down_send, down_recv, give_send, give_recv,
    core_send, core_recv, stage_send, stage_recv, last_send, last_recv,
):
    my_row, my_col = lax.axis_index("row"), lax.axis_index("col")
    bits = n_col.bit_length() - 1
    side = lax.rem(my_col, 2)
    partner = my_col + 1 - 2 * side
    above = jnp.minimum(my_row + 1, n_row - 1)
    below = jnp.maximum(my_row - 1, 0)
    a_parts = (a0, a1)
    chunks = length // SPAN
    parts = [(b_low, MOST, 0, LOW)]
    if chunks > LOW:
        parts.append((b_high, length - MOST, LOW, chunks))
    once = length == MOST
    shared = length if once else 2 * length - 2 * MOST
    first_shared = shared // SPAN
    delay = SKEW * (n_row - 1)

    def flip(bit):
        on = lax.rem(lax.div(my_col, 1 << bit), 2)
        return my_col + (1 << bit) - 2 * on * (1 << bit)

    choice = pltpu.make_async_copy(sections_in, sections, brief)
    number = pltpu.make_async_copy(sums, totals, tiny)
    choice.start()
    number.start()
    greet(n_row, n_col, my_row, my_col)
    along_row, along_col = gathering(
        n_row, n_col, my_row, my_col, flags, every, row_send, row_recv, col_send, col_recv
    )
    own = pltpu.make_async_copy(flags, every.at[my_col, my_row], local)
    choice.wait()
    number.wait()
    tags = [sections[s] for s in range(SECTIONS)]
    owners = [lax.div(tag, ratio) for tag in tags]

    def up(ref, size, g, c):
        part = pl.ds(c * SPAN, SPAN)
        return send(ref.at[part], ref.at[part], up_send.at[g], up_recv.at[g], above, my_col)

    def down(ref, size, g, c):
        part = pl.ds(size + c * SPAN, SPAN)
        return send(ref.at[part], ref.at[part], down_send.at[g], down_recv.at[g], below, my_col)

    def core_swap():
        return send(own_a.at[pl.ds((1 - side) * HALF, HALF)], swapped, core_send, core_recv, my_row, partner)

    def pal_swap():
        return send(own_b.at[pl.ds(MOST, MOST)], pal, pal_send, pal_recv, my_row, partner)

    def hand(c):
        part = pl.ds(c * SPAN, SPAN)
        return send(give.at[part], got_back.at[part], give_send.at[c], give_recv.at[c], my_row, partner)

    def stage(bit, j):
        src = held if bit == 1 else stages.at[bit - 2]
        part = pl.ds(j * A_SPAN, A_SPAN)
        return send(
            src.at[part], stages.at[bit - 1, part], stage_send.at[bit - 1, j], stage_recv.at[bit - 1, j],
            my_row, flip(bit),
        )

    def last(s, j):
        part = pl.ds(side * HALF + j * A_SPAN, A_SPAN)
        i = s * A_STEPS + j
        return send(a_parts[s].at[part], a_parts[s].at[part], last_send.at[i], last_recv.at[i], my_row, partner)

    core_swap().start()
    if not once:
        pal_swap().start()
    own.start()
    for k in range(1, n_row):
        along_row(k).start()

    again = tags[0] == tags[1]
    count = totals[my_col, 0, 0]
    pal_count = totals[partner, 0, 0]
    filled = count + jnp.where(again, 0, totals[my_col, 1, 0])
    shift = jnp.where(again, 0, count)

    def listed(slot, with_pal):
        at = jnp.where(slot < count, slot, MOST + jnp.clip(slot - count, 0, MOST - 1))
        if not with_pal:
            return own_b[at]
        from_pal = jnp.clip(2 * length - 1 - slot - pal_count, 0, MOST - 1)
        return jnp.where(slot < filled, own_b[at], pal[from_pal])

    def parted(g, body):
        for ref, size, begins, ends in parts:

            @pl.when((g >= begins) & (g < ends))
            def _():
                body(ref, size, g, g - begins)

    def feed(way, region, with_pal, ref, size, g, c):
        for k in range(SPAN):
            ref[region * size + c * SPAN + k] = listed(g * SPAN + k, with_pal)
        way(ref, size, g, c).start()

    def take(way, region, onward, with_pal, ref, size, g, c):
        way(ref, size, g, c).wait_recv()
        for k in range(SPAN):
            slot = g * SPAN + k
            spot = region * size + c * SPAN + k
            mine = jnp.where(slot < count, owners[0], owners[1]) == my_row
            ref[spot] = jnp.where(mine, listed(slot, with_pal), ref[spot])

        @pl.when(onward)
        def _():
            way(ref, size, g, c).start()

    def lower_of(s):
        return (owners[s] >= my_row) & (my_row < n_row - 1)

    def hand_over(ref, size, g, c):
        for k in range(SPAN):
            here = c * SPAN + k
            got = jnp.where(lower_of(1), ref[size + here], ref[here])
            give[g * SPAN + k - shared] = got
        hand(g - first_shared).start()

    def hop(i, with_pal):
        @pl.when(my_row == 0)
        def _():
            parted(i, functools.partial(feed, up, 0, with_pal))

        @pl.when(my_row == n_row - 1)
        def _():
            parted(i, functools.partial(feed, down, 1, with_pal))

        @pl.when(my_row > 0)
        def _():
            parted(i - SKEW * my_row, functools.partial(take, up, 0, my_row < n_row - 1, with_pal))

        @pl.when(my_row < n_row - 1)
        def _():
            parted(i - SKEW * (n_row - 1 - my_row), functools.partial(take, down, 1, my_row > 0, with_pal))

        if with_pal and first_shared < chunks:

            @pl.when(i - delay >= first_shared)
            def _():
                parted(i - delay, hand_over)

    def pass_a(bit, j):
        stage(bit, j).wait_recv()
        final = bit == bits - 1
        for s in range(SECTIONS):

            @pl.when((j >= s * A_STEPS) & (j < (s + 1) * A_STEPS))
            def _():
                near = lax.div(tags[s], 1 << bit) == lax.div(my_col, 1 << bit)
                for k in range(A_SPAN):
                    i = j * A_SPAN + k
                    before = held[i] if bit == 1 else stages[bit - 2, i]
                    got = jnp.where(near, before, stages[bit - 1, i])
                    if final:
                        a_parts[s][side * HALF + i - s * HALF] = got
                    else:
                        stages[bit - 1, i] = got
                if final:
                    last(s, j - s * A_STEPS).start()

        if not final:
            stage(bit + 1, j).start()

    lag = 4

    def pass_all(i):
        for bit in range(1, bits):
            j2 = i - lag * bit

            @pl.when((j2 >= 0) & (j2 < 2 * SECTIONS * A_STEPS) & (lax.rem(j2, 2) == 0))
            def _():
                pass_a(bit, lax.div(j2, 2))

    def step(i, with_pal=True):
        hop(i, with_pal)
        pass_all(i)

    def send_a():
        core_swap().wait_recv()
        for s in range(SECTIONS):
            mine = tags[s] == my_col

            @pl.loop(0, HALF)
            def _(k):
                held[s * HALF + k] = jnp.where(mine, own_a[side * HALF + k], swapped[k])

        @pl.loop(0, SECTIONS * A_STEPS)
        def _(j):
            stage(1, j).start()

    start = LOW + delay
    early = min(first_shared, start - 16)
    opening = 2

    def survey():
        for k in range(1, n_col):
            along_col(k).wait_recv()
        for s in range(SECTIONS):
            staged[s, 0] = every[tags[s], my_row, 0]
            staged[s, 1] = every[my_col, owners[s], 1 + lax.rem(tags[s], ratio)]
        tables = pltpu.make_async_copy(staged, table, local)
        tables.start()
        sides = []
        for s in range(SECTIONS):
            rows = [every[tags[s], r, 0].astype(jnp.float32).T[0:tile_rows] for r in range(n_row)]
            sides.append(jnp.concatenate(rows, axis=0))
        blocks = lax.broadcasted_iota(jnp.int32, (n_row * tile_rows, TILE), 0) // tile_rows * n_col
        me = my_row * n_col + my_col
        lower = jnp.zeros((n_row * tile_rows, TILE), jnp.float32)
        chosen = jnp.zeros((n_row * tile_rows, TILE), jnp.float32)
        for c in range(n_col):
            common = jnp.zeros((n_row * tile_rows, TILE), jnp.float32)
            for s in range(SECTIONS):
                tile_flags = every[c, owners[s], 1 + lax.rem(tags[s], ratio)].astype(jnp.float32)
                common += jnp.dot(sides[s], tile_flags, preferred_element_type=jnp.float32)
            occupied = jnp.where(common > 0.5, 1.0, 0.0)
            lower += jnp.where(blocks + c < me, occupied, 0.0)
            chosen += jnp.where(my_col == c, occupied, 0.0)
        occ[...] = chosen
        offset = jnp.sum(jnp.sum(lower, axis=1, keepdims=True), axis=0, keepdims=True)
        mine = pl.ds(pl.multiple_of(my_row * tile_rows, tile_rows), tile_rows)
        meta[0:tile_rows] = occ[mine].astype(jnp.int32)
        meta[tile_rows:] = jnp.broadcast_to(offset, (8, TILE)).astype(jnp.int32)

        tables.wait()
        for s in range(SECTIONS):

            def lap_a(p, rank):
                begin[s, 0, p] = rank
                for q in range(panel):
                    rank = rank + table[s, 0, q, p]
                return rank

            def lap_b(p, rank):
                begin[s, 1, p] = rank
                for q in range(tile_cols):
                    rank = rank + table[s, 1, p, q]
                return rank

            lax.fori_loop(0, tile_rows, lap_a, jnp.int32(0))
            lax.fori_loop(0, panel, lap_b, jnp.int32(0))

    def relay():
        own.wait()
        for k in range(1, n_row):
            along_row(k).wait_recv()
        for k in range(1, n_col):
            along_col(k).start()

    @pl.loop(0, early)
    def _(i):
        step(i, False)

        @pl.when(i == opening)
        def _():
            relay()
            send_a()

    if not once:
        pal_swap().wait_recv()

    def put(ref, p, cols, rank, flag_at, load):
        for q in range(cols):
            here = flag_at(q)
            got = load(rank)
            tile_at(ref, p, q)[...] = jnp.where(here == 1, got, jnp.zeros_like(got))
            rank = rank + here

    double = tile_rows // panel

    def spread_a(s, u):
        for k in range(double):
            p = u * double + k
            put(
                a_full, p, panel, begin[s, 0, p], lambda q: table[s, 0, q, p],
                lambda rank: a_parts[s][jnp.minimum(rank, MOST - 1)],
            )

    def spread_b0(p):
        base = jnp.where(lower_of(0), MOST, 0)
        put(
            b_full, p, tile_cols, begin[0, 1, p], lambda q: table[0, 1, p, q],
            lambda rank: b_low[base + jnp.minimum(rank, MOST - 1)],
        )

    def spread_b1(p):
        low = lower_of(1)

        def load(rank):
            place = shift + rank
            got = b_low[jnp.where(low, MOST, 0) + jnp.minimum(place, MOST - 1)]
            if length > MOST:
                size = length - MOST
                at = jnp.where(low, size, 0) + jnp.clip(place - MOST, 0, size - 1)
                got = jnp.where(place < MOST, got, b_high[at])
            if shared < length:
                got = jnp.where(place < length, got, got_back[jnp.clip(2 * MOST - 1 - place, 0, length - shared - 1)])
            return got

        put(b_full, p, tile_cols, begin[1, 1, p], lambda q: table[1, 1, p, q], load)

    across = tile_cols * TILE // BLOCK
    pieces = across * (tile_rows * TILE // BLOCK)

    def multiply(j):
        rows, cols = block_at(lax.div(j, across)), block_at(lax.rem(j, across))
        return rows, cols, jnp.dot(a_full[rows, :], b_full[:, cols], preferred_element_type=jnp.float32)

    def multiply_first(j):
        rows, cols, got = multiply(j)
        acc[rows, cols] = got

    def a_here(s):
        for j in range(A_STEPS):
            last(s, j).wait_recv()

    spare = chunks - LOW
    light = spare // 8
    plan = [(start - panel, panel, panel, lambda: a_here(0), functools.partial(spread_a, 0))]
    if once:
        plan.append((start, 0, panel, None, spread_b0))
    else:
        plan.append((start, light, panel, None, spread_b0))
        plan.append((start + light, spare - 2 * light, pieces, None, multiply_first))
        plan.append((start + spare - light, light, panel, lambda: a_here(1), functools.partial(spread_a, 1)))

    @pl.loop(early, chunks + delay)
    def _(i):
        step(i)

        @pl.when(i == early + 1)
        def _():
            survey()

        for begins, steps, units, before, body in plan:
            if steps:
                per = -(-units // steps)
                c = i - begins

                @pl.when((c >= 0) & (c < steps))
                def _():
                    if before is not None:

                        @pl.when(c == 0)
                        def _():
                            before()

                    @pl.loop(c * per, jnp.minimum((c + 1) * per, units))
                    def _(u):
                        body(u)

    for begins, steps, units, before, body in plan:
        if not steps:
            if before is not None:
                before()

            @pl.loop(0, units)
            def _(u):
                body(u)

    if first_shared < chunks:

        @pl.loop(0, chunks - first_shared)
        def _(c):
            hand(c).wait_recv()

    if once:
        a_here(1)
    else:

        @pl.loop(0, panel)
        def _(p):
            spread_b1(p)

    @pl.loop(0, pieces)
    def _(j):
        rows, cols, got = multiply(j)
        done[rows, cols] = (got + got if once else acc[rows, cols] + got).astype(done.dtype)

    for k in range(1, n_row):
        along_row(k).wait_send()
    for k in range(1, n_col):
        along_col(k).wait_send()
    if not once:
        pal_swap().wait_send()
    core_swap().wait_send()
    if first_shared < chunks:

        @pl.loop(0, chunks - first_shared)
        def _(c):
            hand(c).wait_send()

    for s in range(SECTIONS):

        @pl.loop(0, A_STEPS)
        def _(j):
            last(s, j).wait_send()

    for ref, size, begins, ends in parts:

        @pl.loop(begins, ends)
        def _(g):
            @pl.when(my_row < n_row - 1)
            def _():
                up(ref, size, g, g - begins).wait_send()

            @pl.when(my_row > 0)
            def _():
                down(ref, size, g, g - begins).wait_send()

    for bit in range(1, bits):

        @pl.loop(0, SECTIONS * A_STEPS)
        def _(j):
            stage(bit, j).wait_send()


def final_kernel(tile_rows, tile_cols, meta_in, done, out, places, meta, zero, local, sem):
    load = pltpu.make_async_copy(meta_in, meta, local)
    load.start()
    zero[...] = jnp.zeros_like(zero)
    load.wait()

    def lap(p, rank):
        for q in range(tile_cols):
            here = meta[p, q]

            @pl.when(here == 1)
            def _():
                spot = tile_at(out, lax.div(rank, tile_cols), lax.rem(rank, tile_cols))
                pltpu.make_async_copy(tile_at(done, p, q), spot, sem).start()

            rank = rank + here
        return rank

    filled = lax.fori_loop(0, tile_rows, lap, jnp.int32(0))

    @pl.loop(filled, tile_rows * tile_cols)
    def _(k):
        pltpu.make_async_copy(zero, tile_at(out, lax.div(k, tile_cols), lax.rem(k, tile_cols)), sem).start()

    down_slots = lax.broadcasted_iota(jnp.int32, places.shape, 0) * tile_cols
    slot = down_slots + lax.broadcasted_iota(jnp.int32, places.shape, 1)
    places[...] = jnp.where(slot < filled, meta[tile_rows, 0] + slot, -1)
    pltpu.make_async_copy(done, out, sem).wait()


def in_hbm(x):
    return pltpu.with_memory_space_constraint(x, pltpu.HBM)


def in_vmem(x):
    return pltpu.with_memory_space_constraint(x, pltpu.VMEM)


def shards(n_row, n_col, a_matrix, a_flags, b_matrix, b_flags, sections):
    tile_rows, panel = a_flags.shape
    tile_cols = b_flags.shape[1]
    ratio = n_col // n_row
    dtype = a_matrix.dtype
    bits = n_col.bit_length() - 1
    dma = pltpu.SemaphoreType.DMA

    def tiles(*lead):
        return lead + (TILE, TILE)

    size = (tile_rows * TILE, tile_cols * TILE)
    sums, pick = pl.pallas_call(
        functools.partial(count_kernel, n_row, n_col, ratio),
        out_shape=(
            jax.ShapeDtypeStruct((n_col, SECTIONS, TILE), jnp.int32), jax.ShapeDtypeStruct((1, TILE), jnp.int32)
        ),
        in_specs=[HBM, HBM],
        out_specs=(VMEM, VMEM),
        scratch_shapes=[
            pltpu.VMEM((SECTIONS, TILE), jnp.int32),
            pltpu.VMEM((ratio, panel, tile_cols), jnp.int32),
            pltpu.VMEM((n_col, n_row, SECTIONS, TILE), jnp.int32),
            pltpu.SMEM((SECTIONS,), jnp.int32), dma, dma, dma((n_row,)), dma((n_row,)), dma((n_col,)), dma((n_col,))
        ],
        compiler_params=pltpu.CompilerParams(
            collective_id=len(LENGTHS), has_side_effects=True, vmem_limit_bytes=8 * 1024 * 1024
        ),
        name="counts",
    )(in_hbm(sections), in_hbm(b_flags.reshape(ratio, panel, tile_cols)))

    def exchange(level, sections, a_flags, b_flags, a, b, sums):
        own_a, own_b, flags = pl.pallas_call(
            functools.partial(pack_kernel, tile_rows, panel, tile_cols, ratio),
            out_shape=(
                pltpu.VMEM(tiles(MOST), dtype),
                pltpu.VMEM(tiles(SECTIONS * MOST), dtype),
                pltpu.VMEM((1 + ratio, panel, TILE), jnp.int32),
            ),
            in_specs=[HBM] * 5,
            out_specs=(VMEM,) * 3,
            scratch_shapes=[
                pltpu.SMEM((SECTIONS,), jnp.int32),
                pltpu.SMEM((panel, tile_rows), jnp.int32),
                pltpu.SMEM(b_flags.shape, jnp.int32),
                pltpu.VMEM((panel, tile_rows), jnp.int32),
                pltpu.VMEM(b_flags.shape, jnp.int32),
                dma((5,)), dma,
            ],
            compiler_params=pltpu.CompilerParams(vmem_limit_bytes=16 * 1024 * 1024),
            name="pack",
        )(*[in_hbm(x) for x in (sections, a_flags, b_flags, a, b)])

        length = LENGTHS[level]
        chunks = length // SPAN
        handed = SPAN if level == 0 else max(2 * MOST - length, SPAN)
        done, meta = pl.pallas_call(
            functools.partial(comm_kernel, length, n_row, n_col, tile_rows, panel, tile_cols, ratio),
            out_shape=(
                pltpu.VMEM(size, dtype),
                pltpu.VMEM((tile_rows + 8, TILE), jnp.int32),
            ),
            in_specs=[HBM, VMEM, VMEM, VMEM, HBM],
            out_specs=(VMEM,) * 2,
            scratch_shapes=[
                pltpu.SMEM((SECTIONS,), jnp.int32),
                pltpu.SMEM((n_col, SECTIONS, TILE), jnp.int32),
                pltpu.VMEM((n_col, n_row, 1 + ratio, panel, TILE), jnp.int32),
                pltpu.VMEM((SECTIONS, 2, panel, TILE), jnp.int32),
                pltpu.SMEM((SECTIONS, 2, panel, TILE), jnp.int32),
                pltpu.SMEM((SECTIONS, 2, tile_rows), jnp.int32),
                pltpu.VMEM((n_row * tile_rows, TILE), jnp.float32),
                pltpu.VMEM(tiles(HALF), dtype),
                pltpu.VMEM(tiles(MOST), dtype),
                pltpu.VMEM(tiles(MOST), dtype),
                pltpu.VMEM(tiles(MOST), dtype),
                pltpu.VMEM(tiles(2 * MOST), dtype),
                pltpu.VMEM(tiles(2 * max(length - MOST, 1)), dtype),
                pltpu.VMEM(tiles(MOST), dtype),
                pltpu.VMEM(tiles(handed), dtype),
                pltpu.VMEM(tiles(handed), dtype),
                pltpu.VMEM(tiles(bits - 1, MOST), dtype),
                pltpu.VMEM(size if level else (8, TILE), jnp.float32),
                pltpu.VMEM((tile_rows * TILE, panel * TILE), dtype),
                pltpu.VMEM((panel * TILE, tile_cols * TILE), dtype),
                dma, dma, dma, dma, dma, dma((n_row,)), dma((n_row,)), dma((n_col,)), dma((n_col,)),
                dma((chunks,)), dma((chunks,)), dma((chunks,)), dma((chunks,)),
                dma((handed // SPAN,)), dma((handed // SPAN,)),
                dma, dma,
                dma((bits - 1, SECTIONS * A_STEPS)), dma((bits - 1, SECTIONS * A_STEPS)),
                dma((SECTIONS * A_STEPS,)), dma((SECTIONS * A_STEPS,)),
            ],
            compiler_params=pltpu.CompilerParams(
                collective_id=level, has_side_effects=True, vmem_limit_bytes=49 * 1024 * 1024
            ),
            name=f"exchange_{length}",
        )(in_hbm(sections), *[in_vmem(x) for x in (own_a, own_b, flags)], in_hbm(sums))

        return pl.pallas_call(
            functools.partial(final_kernel, tile_rows, tile_cols),
            out_shape=(jax.ShapeDtypeStruct(size, dtype), jax.ShapeDtypeStruct((tile_rows, tile_cols), jnp.int32)),
            in_specs=[VMEM] * 2,
            out_specs=(HBM, VMEM),
            scratch_shapes=[
                pltpu.SMEM(meta.shape, jnp.int32), pltpu.VMEM((TILE, TILE), dtype), dma, dma
            ],
            compiler_params=pltpu.CompilerParams(vmem_limit_bytes=12 * 1024 * 1024),
            name="compact",
        )(*[in_vmem(x) for x in (meta, done)])

    branches = [functools.partial(exchange, level) for level in range(len(LENGTHS))]
    return lax.switch(pick[0, 0], branches, sections, a_flags.T, b_flags, a_matrix, b_matrix, sums)


def solution(mesh):
    return jax.shard_map(
        functools.partial(shards, mesh.shape["row"], mesh.shape["col"]),
        mesh=mesh,
        in_specs=(P("row", "col"), P("row", "col"), P("row", "col"), P("row", "col"), P()),
        out_specs=(P("row", "col"), P("row", "col")),
        check_vma=False,
    )
```

```python
import functools

import jax
import jax.numpy as jnp
from jax import lax
from jax.experimental import pallas as pl
from jax.experimental.pallas import tpu as pltpu
from jax.sharding import PartitionSpec as P

TILE = 128
SECTIONS = 2
MOST = 64
HALF = MOST // 2
SPAN = 2
LOW = MOST // SPAN
LENGTHS = (64, 80, 88, 96, 104, 112, 128)
A_SPAN = 4
A_STEPS = HALF // A_SPAN
BLOCK = 512
SKEW = 3
FIRST_LAG = 10
LAG = 6
MESH = pl.DeviceIdType.MESH
HBM = pl.BlockSpec(memory_space=pltpu.HBM)
SMEM = pl.BlockSpec(memory_space=pltpu.SMEM)
VMEM = pl.BlockSpec(memory_space=pltpu.VMEM)


def tile_at(ref, p, q):
    rows = pl.ds(pl.multiple_of(p * TILE, TILE), TILE)
    cols = pl.ds(q * TILE if isinstance(q, int) else pl.multiple_of(q * TILE, TILE), TILE)
    return ref.at[rows, cols]


def block_at(j, size=BLOCK):
    return pl.ds(pl.multiple_of(j * size, size), size)


def pack_kernel(
    tile_rows, panel, tile_cols, ratio, sections_in, a_flags_in, b_flags_in, a, b,
    a_out, b_out, flags, sections, a_flags, b_flags, a_vec, b_vec, sems, sem,
):
    moves = (
        (sections_in, sections), (b_flags_in, b_flags), (a_flags_in, a_flags), (a_flags_in, a_vec), (b_flags_in, b_vec)
    )
    loads = [pltpu.make_async_copy(src, dst, sems.at[i]) for i, (src, dst) in enumerate(moves)]
    for load in loads:
        load.start()
    flags[...] = jnp.zeros_like(flags)
    for load in loads:
        load.wait()

    def gather(occupied, src, out, base, rows, cols, first, turned):
        def lap(p, rank):
            for q in range(cols):
                here = occupied[q, p] if turned else occupied[first + p, q]

                @pl.when(here == 1)
                def _():
                    pltpu.make_async_copy(tile_at(src, first + p, q), out.at[base + rank], sem).start()

                rank = rank + here
            return rank

        return lax.fori_loop(0, rows, lap, jnp.int32(0))

    total = jnp.int32(0)
    my_row, my_col = lax.axis_index("row"), lax.axis_index("col")
    mine_a = (sections[0] == my_col) | (sections[1] == my_col)
    for s in range(SECTIONS):
        first = lax.rem(sections[s], ratio) * panel
        total += lax.cond(
            sections[s] // ratio == my_row,
            lambda: gather(b_flags, b, b_out, s * MOST, panel, tile_cols, first, False),
            lambda: jnp.int32(0),
        )
    total += lax.cond(mine_a, lambda: gather(a_flags, a, a_out, 0, tile_rows, panel, 0, True), lambda: jnp.int32(0))

    flags[0, :, 0:tile_rows] = a_vec[...]
    for i in range(ratio):
        flags[1 + i, :, 0:tile_cols] = b_vec[i * panel : (i + 1) * panel, :]

    @pl.loop(0, total)
    def _(i):
        pltpu.make_async_copy(tile_at(a, 0, 0), a_out.at[0], sem).wait()


def count_kernel(
    n_row, n_col, ratio, sections_in, b_flags, sums, pick,
    counts, b_vec, every, sections, local, brief, row_send, row_recv, col_send, col_recv,
):
    my_row, my_col = lax.axis_index("row"), lax.axis_index("col")
    choice = pltpu.make_async_copy(sections_in, sections, brief)
    load = pltpu.make_async_copy(b_flags, b_vec, local)
    choice.start()
    load.start()
    greet(n_row, n_col, my_row, my_col)
    choice.wait()
    load.wait()
    for s in range(SECTIONS):
        found = b_vec[lax.rem(sections[s], ratio)].astype(jnp.float32)
        found = jnp.sum(jnp.sum(found, axis=1, keepdims=True), axis=0, keepdims=True)
        found = jnp.where(lax.div(sections[s], ratio) == my_row, found, jnp.zeros_like(found))
        counts[s : s + 1, :] = jnp.broadcast_to(found, (1, TILE)).astype(jnp.int32)
    along_row, along_col = gathering(
        n_row, n_col, my_row, my_col, counts, every, row_send, row_recv, col_send, col_recv
    )
    for k in range(1, n_row):
        along_row(k).start()
    own = pltpu.make_async_copy(counts, every.at[my_col, my_row], local)
    own.start()
    own.wait()
    for k in range(1, n_row):
        along_row(k).wait_recv()
    for k in range(1, n_col):
        along_col(k).start()
    for k in range(1, n_col):
        along_col(k).wait_recv()

    again = sections[0] == sections[1]
    weight = jnp.where(again, 0, 1)
    most = jnp.zeros((1, TILE), jnp.int32)
    for c in range(0, n_col, 2):
        pair = jnp.zeros((1, TILE), jnp.int32)
        for d in (c, c + 1):
            whole = sum(every[d, r] for r in range(n_row))
            sums[d] = whole
            pair += whole[0:1] + whole[1:2] * weight
        most = jnp.maximum(most, pair)
    level = 1 + sum(jnp.where(most > 2 * length, 1, 0) for length in LENGTHS[1:-1])
    pick[...] = jnp.where(again, 0, level)

    for k in range(1, n_row):
        along_row(k).wait_send()
    for k in range(1, n_col):
        along_col(k).wait_send()


def greet(n_row, n_col, my_row, my_col):
    barrier = pltpu.get_barrier_semaphore()
    for k in range(1, n_row):
        pl.semaphore_signal(barrier, inc=1, device_id=(lax.rem(my_row + k, n_row), my_col), device_id_type=MESH)
    for k in range(1, n_col):
        pl.semaphore_signal(barrier, inc=1, device_id=(my_row, lax.rem(my_col + k, n_col)), device_id_type=MESH)
    pl.semaphore_wait(barrier, n_row + n_col - 2)


def gathering(n_row, n_col, my_row, my_col, mine, every, row_send, row_recv, col_send, col_recv):
    def along_row(k):
        return send(
            mine, every.at[my_col, my_row], row_send.at[k], row_recv.at[k], lax.rem(my_row + k, n_row), my_col
        )

    def along_col(k):
        return send(
            every.at[my_col], every.at[my_col], col_send.at[k], col_recv.at[k], my_row, lax.rem(my_col + k, n_col)
        )

    return along_row, along_col


def send(src, dst, send_sem, recv_sem, row, col):
    return pltpu.make_async_remote_copy(
        src_ref=src, dst_ref=dst, send_sem=send_sem, recv_sem=recv_sem, device_id=(row, col), device_id_type=MESH
    )


def comm_kernel(
    length, n_row, n_col, tile_rows, panel, tile_cols, ratio,
    sections_in, own_a, own_b, flags, sums, done, meta,
    sections, totals, every, staged, table, begin, occ, swapped, held, a0, a1, b_low, b_high, pal, give, got_back, stages,
    acc, a_full, b_full,
    local, brief, tiny, pal_send, pal_recv, row_send, row_recv, col_send, col_recv,
    up_send, up_recv, down_send, down_recv, give_send, give_recv,
    core_send, core_recv, stage_send, stage_recv, last_send, last_recv,
):
    my_row, my_col = lax.axis_index("row"), lax.axis_index("col")
    bits = n_col.bit_length() - 1
    side = lax.rem(my_col, 2)
    partner = my_col + 1 - 2 * side
    above = jnp.minimum(my_row + 1, n_row - 1)
    below = jnp.maximum(my_row - 1, 0)
    a_parts = (a0, a1)
    chunks = length // SPAN
    parts = [(b_low, MOST, 0, LOW)]
    if chunks > LOW:
        parts.append((b_high, length - MOST, LOW, chunks))
    once = length == MOST
    a_sections = 1 if once else SECTIONS
    shared = length if once else 2 * length - 2 * MOST
    first_shared = shared // SPAN
    delay = SKEW * (n_row - 1)

    def flip(bit):
        on = lax.rem(lax.div(my_col, 1 << bit), 2)
        return my_col + (1 << bit) - 2 * on * (1 << bit)

    choice = pltpu.make_async_copy(sections_in, sections, brief)
    number = pltpu.make_async_copy(sums, totals, tiny)
    choice.start()
    number.start()
    greet(n_row, n_col, my_row, my_col)
    along_row, along_col = gathering(
        n_row, n_col, my_row, my_col, flags, every, row_send, row_recv, col_send, col_recv
    )
    own = pltpu.make_async_copy(flags, every.at[my_col, my_row], local)
    choice.wait()
    number.wait()
    tags = [sections[s] for s in range(SECTIONS)]
    owners = [lax.div(tag, ratio) for tag in tags]

    def up(ref, size, g, c):
        part = pl.ds(c * SPAN, SPAN)
        return send(ref.at[part], ref.at[part], up_send.at[g], up_recv.at[g], above, my_col)

    def down(ref, size, g, c):
        part = pl.ds(size + c * SPAN, SPAN)
        return send(ref.at[part], ref.at[part], down_send.at[g], down_recv.at[g], below, my_col)

    def core_swap():
        return send(own_a.at[pl.ds((1 - side) * HALF, HALF)], swapped, core_send, core_recv, my_row, partner)

    def pal_swap():
        return send(own_b.at[pl.ds(MOST, MOST)], pal, pal_send, pal_recv, my_row, partner)

    def hand(c):
        part = pl.ds(c * SPAN, SPAN)
        return send(give.at[part], got_back.at[part], give_send.at[c], give_recv.at[c], my_row, partner)

    def stage(bit, j):
        src = held if bit == 1 else stages.at[bit - 2]
        part = pl.ds(j * A_SPAN, A_SPAN)
        return send(
            src.at[part], stages.at[bit - 1, part], stage_send.at[bit - 1, j], stage_recv.at[bit - 1, j],
            my_row, flip(bit),
        )

    def last(s, j):
        part = pl.ds(side * HALF + j * A_SPAN, A_SPAN)
        i = s * A_STEPS + j
        return send(a_parts[s].at[part], a_parts[s].at[part], last_send.at[i], last_recv.at[i], my_row, partner)

    core_swap().start()
    if not once:
        pal_swap().start()
    own.start()
    for k in range(1, n_row):
        along_row(k).start()

    again = tags[0] == tags[1]
    count = totals[my_col, 0, 0]
    pal_count = totals[partner, 0, 0]
    filled = count + jnp.where(again, 0, totals[my_col, 1, 0])
    shift = jnp.where(again, 0, count)

    def listed(slot, with_pal):
        at = jnp.where(slot < count, slot, MOST + jnp.clip(slot - count, 0, MOST - 1))
        if not with_pal:
            return own_b[at]
        from_pal = jnp.clip(2 * length - 1 - slot - pal_count, 0, MOST - 1)
        return jnp.where(slot < filled, own_b[at], pal[from_pal])

    def parted(g, body):
        for ref, size, begins, ends in parts:

            @pl.when((g >= begins) & (g < ends))
            def _():
                body(ref, size, g, g - begins)

    def feed(way, region, with_pal, ref, size, g, c):
        for k in range(SPAN):
            ref[region * size + c * SPAN + k] = listed(g * SPAN + k, with_pal)
        way(ref, size, g, c).start()

    def take(way, region, onward, with_pal, ref, size, g, c):
        way(ref, size, g, c).wait_recv()
        for k in range(SPAN):
            slot = g * SPAN + k
            spot = region * size + c * SPAN + k
            mine = jnp.where(slot < count, owners[0], owners[1]) == my_row
            ref[spot] = jnp.where(mine, listed(slot, with_pal), ref[spot])

        @pl.when(onward)
        def _():
            way(ref, size, g, c).start()

    def lower_of(s):
        return (owners[s] >= my_row) & (my_row < n_row - 1)

    def hand_over(ref, size, g, c):
        for k in range(SPAN):
            here = c * SPAN + k
            got = jnp.where(lower_of(1), ref[size + here], ref[here])
            give[g * SPAN + k - shared] = got
        hand(g - first_shared).start()

    def hop(i, with_pal):
        @pl.when(my_row == 0)
        def _():
            parted(i, functools.partial(feed, up, 0, with_pal))

        @pl.when(my_row == n_row - 1)
        def _():
            parted(i, functools.partial(feed, down, 1, with_pal))

        @pl.when(my_row > 0)
        def _():
            parted(i - SKEW * my_row, functools.partial(take, up, 0, my_row < n_row - 1, with_pal))

        @pl.when(my_row < n_row - 1)
        def _():
            parted(i - SKEW * (n_row - 1 - my_row), functools.partial(take, down, 1, my_row > 0, with_pal))

        if with_pal and first_shared < chunks:

            @pl.when(i - delay >= first_shared)
            def _():
                parted(i - delay, hand_over)

    def pass_a(bit, j):
        stage(bit, j).wait_recv()
        final = bit == bits - 1
        for s in range(a_sections):

            @pl.when((j >= s * A_STEPS) & (j < (s + 1) * A_STEPS))
            def _():
                near = lax.div(tags[s], 1 << bit) == lax.div(my_col, 1 << bit)
                for k in range(A_SPAN):
                    i = j * A_SPAN + k
                    before = held[i] if bit == 1 else stages[bit - 2, i]
                    got = jnp.where(near, before, stages[bit - 1, i])
                    if final:
                        a_parts[s][side * HALF + i - s * HALF] = got
                    else:
                        stages[bit - 1, i] = got
                if final:
                    last(s, j - s * A_STEPS).start()

        if not final:
            stage(bit + 1, j).start()

    def pass_all(i):
        for bit in range(1, bits):
            j2 = i - FIRST_LAG - LAG * (bit - 1)

            @pl.when((j2 >= 0) & (j2 < 2 * a_sections * A_STEPS) & (lax.rem(j2, 2) == 0))
            def _():
                pass_a(bit, lax.div(j2, 2))

    def step(i, with_pal=True):
        hop(i, with_pal)
        pass_all(i)

    def send_a():
        core_swap().wait_recv()
        for s in range(a_sections):
            mine = tags[s] == my_col

            @pl.loop(0, HALF)
            def _(k):
                held[s * HALF + k] = jnp.where(mine, own_a[side * HALF + k], swapped[k])

        @pl.loop(0, a_sections * A_STEPS)
        def _(j):
            stage(1, j).start()

    start = LOW + delay
    early = min(first_shared, start - 16)
    opening = 2

    def tables():
        return pltpu.make_async_copy(staged, table, local)

    def survey():
        for k in range(1, n_col):
            along_col(k).wait_recv()
        for s in range(SECTIONS):
            staged[s, 0] = every[tags[s], my_row, 0]
            staged[s, 1] = every[my_col, owners[s], 1 + lax.rem(tags[s], ratio)]
        tables().start()

    def survey_tiles():
        sides = []
        for s in range(SECTIONS):
            rows = [every[tags[s], r, 0].astype(jnp.float32).T[0:tile_rows] for r in range(n_row)]
            sides.append(jnp.concatenate(rows, axis=0))
        blocks = lax.broadcasted_iota(jnp.int32, (n_row * tile_rows, TILE), 0) // tile_rows * n_col
        me = my_row * n_col + my_col
        lower = jnp.zeros((n_row * tile_rows, TILE), jnp.float32)
        chosen = jnp.zeros((n_row * tile_rows, TILE), jnp.float32)
        for c in range(n_col):
            common = jnp.zeros((n_row * tile_rows, TILE), jnp.float32)
            for s in range(SECTIONS):
                tile_flags = every[c, owners[s], 1 + lax.rem(tags[s], ratio)].astype(jnp.float32)
                common += jnp.dot(sides[s], tile_flags, preferred_element_type=jnp.float32)
            occupied = jnp.where(common > 0.5, 1.0, 0.0)
            lower += jnp.where(blocks + c < me, occupied, 0.0)
            chosen += jnp.where(my_col == c, occupied, 0.0)
        occ[...] = chosen
        offset = jnp.sum(jnp.sum(lower, axis=1, keepdims=True), axis=0, keepdims=True)
        mine = pl.ds(pl.multiple_of(my_row * tile_rows, tile_rows), tile_rows)
        meta[0:tile_rows] = occ[mine].astype(jnp.int32)
        meta[tile_rows:] = jnp.broadcast_to(offset, (8, TILE)).astype(jnp.int32)


    def survey_ranks():
        tables().wait()
        for s in range(SECTIONS):

            def lap_a(p, rank):
                begin[s, 0, p] = rank
                for q in range(panel):
                    rank = rank + table[s, 0, q, p]
                return rank

            def lap_b(p, rank):
                begin[s, 1, p] = rank
                for q in range(tile_cols):
                    rank = rank + table[s, 1, p, q]
                return rank

            lax.fori_loop(0, tile_rows, lap_a, jnp.int32(0))
            lax.fori_loop(0, panel, lap_b, jnp.int32(0))

    def relay():
        own.wait()
        for k in range(1, n_row):
            along_row(k).wait_recv()
        for k in range(1, n_col):
            along_col(k).start()

    @pl.loop(0, early)
    def _(i):
        step(i, False)

        @pl.when(i == opening)
        def _():
            relay()
            send_a()

    if not once:
        pal_swap().wait_recv()

    def put(ref, p, cols, rank, flag_at, load):
        for q in range(cols):
            here = flag_at(q)
            got = load(rank)
            tile_at(ref, p, q)[...] = jnp.where(here == 1, got, jnp.zeros_like(got))
            rank = rank + here

    double = tile_rows // panel

    def spread_a(s, u):
        for k in range(double):
            p = u * double + k
            put(
                a_full, p, panel, begin[s, 0, p], lambda q: table[s, 0, q, p],
                lambda rank: a_parts[s][jnp.minimum(rank, MOST - 1)],
            )

    def spread_b0(p):
        base = jnp.where(lower_of(0), MOST, 0)
        put(
            b_full, p, tile_cols, begin[0, 1, p], lambda q: table[0, 1, p, q],
            lambda rank: b_low[base + jnp.minimum(rank, MOST - 1)],
        )

    def spread_b1(p):
        low = lower_of(1)

        def load(rank):
            place = shift + rank
            got = b_low[jnp.where(low, MOST, 0) + jnp.minimum(place, MOST - 1)]
            if length > MOST:
                size = length - MOST
                at = jnp.where(low, size, 0) + jnp.clip(place - MOST, 0, size - 1)
                got = jnp.where(place < MOST, got, b_high[at])
            if shared < length:
                got = jnp.where(place < length, got, got_back[jnp.clip(2 * MOST - 1 - place, 0, length - shared - 1)])
            return got

        put(b_full, p, tile_cols, begin[1, 1, p], lambda q: table[1, 1, p, q], load)

    across = tile_cols * TILE // BLOCK
    pieces = across * (tile_rows * TILE // BLOCK)

    def multiply(j):
        rows, cols = block_at(lax.div(j, across)), block_at(lax.rem(j, across))
        return rows, cols, jnp.dot(a_full[rows, :], b_full[:, cols], preferred_element_type=jnp.float32)

    def multiply_first(j):
        rows, cols, got = multiply(j)
        acc[rows, cols] = got

    def a_here(s):
        for j in range(A_STEPS):
            last(s, j).wait_recv()

    spare = chunks - LOW
    light = spare // 8
    plan = [(start - panel, panel, panel, lambda: a_here(0), functools.partial(spread_a, 0))]
    if once:
        plan.append((start, 0, panel, None, spread_b0))
    else:
        plan.append((start, light, panel, None, spread_b0))
        plan.append((start + light, spare - 2 * light, pieces, None, multiply_first))
        plan.append((start + spare - light, light, panel, lambda: a_here(1), functools.partial(spread_a, 1)))

    @pl.loop(early, chunks + delay)
    def _(i):
        step(i)

        for k, part in enumerate((survey, survey_ranks, survey_tiles)):

            @pl.when(i == early + 1 + 2 * k)
            def _():
                part()

        for begins, steps, units, before, body in plan:
            if steps:
                per = -(-units // steps)
                c = i - begins

                @pl.when((c >= 0) & (c < steps))
                def _():
                    if before is not None:

                        @pl.when(c == 0)
                        def _():
                            before()

                    @pl.loop(c * per, jnp.minimum((c + 1) * per, units))
                    def _(u):
                        body(u)

    for begins, steps, units, before, body in plan:
        if not steps:
            if before is not None:
                before()

            @pl.loop(0, units)
            def _(u):
                body(u)

    if first_shared < chunks:

        @pl.loop(0, chunks - first_shared)
        def _(c):
            hand(c).wait_recv()

    if not once:

        @pl.loop(0, panel)
        def _(p):
            spread_b1(p)

    @pl.loop(0, pieces)
    def _(j):
        rows, cols, got = multiply(j)
        done[rows, cols] = (got + got if once else acc[rows, cols] + got).astype(done.dtype)

    for k in range(1, n_row):
        along_row(k).wait_send()
    for k in range(1, n_col):
        along_col(k).wait_send()
    if not once:
        pal_swap().wait_send()
    core_swap().wait_send()
    if first_shared < chunks:

        @pl.loop(0, chunks - first_shared)
        def _(c):
            hand(c).wait_send()

    for s in range(a_sections):

        @pl.loop(0, A_STEPS)
        def _(j):
            last(s, j).wait_send()

    for ref, size, begins, ends in parts:

        @pl.loop(begins, ends)
        def _(g):
            @pl.when(my_row < n_row - 1)
            def _():
                up(ref, size, g, g - begins).wait_send()

            @pl.when(my_row > 0)
            def _():
                down(ref, size, g, g - begins).wait_send()

    for bit in range(1, bits):

        @pl.loop(0, a_sections * A_STEPS)
        def _(j):
            stage(bit, j).wait_send()


def final_kernel(tile_rows, tile_cols, meta_in, done, out, places, meta, zero, local, sem):
    load = pltpu.make_async_copy(meta_in, meta, local)
    load.start()
    zero[...] = jnp.zeros_like(zero)
    load.wait()

    def lap(p, rank):
        for q in range(tile_cols):
            here = meta[p, q]

            @pl.when(here == 1)
            def _():
                spot = tile_at(out, lax.div(rank, tile_cols), lax.rem(rank, tile_cols))
                pltpu.make_async_copy(tile_at(done, p, q), spot, sem).start()

            rank = rank + here
        return rank

    filled = lax.fori_loop(0, tile_rows, lap, jnp.int32(0))

    @pl.loop(filled, tile_rows * tile_cols)
    def _(k):
        pltpu.make_async_copy(zero, tile_at(out, lax.div(k, tile_cols), lax.rem(k, tile_cols)), sem).start()

    down_slots = lax.broadcasted_iota(jnp.int32, places.shape, 0) * tile_cols
    slot = down_slots + lax.broadcasted_iota(jnp.int32, places.shape, 1)
    places[...] = jnp.where(slot < filled, meta[tile_rows, 0] + slot, -1)
    pltpu.make_async_copy(done, out, sem).wait()


def in_hbm(x):
    return pltpu.with_memory_space_constraint(x, pltpu.HBM)


def in_vmem(x):
    return pltpu.with_memory_space_constraint(x, pltpu.VMEM)


def shards(n_row, n_col, a_matrix, a_flags, b_matrix, b_flags, sections):
    tile_rows, panel = a_flags.shape
    tile_cols = b_flags.shape[1]
    ratio = n_col // n_row
    dtype = a_matrix.dtype
    bits = n_col.bit_length() - 1
    dma = pltpu.SemaphoreType.DMA

    def tiles(*lead):
        return lead + (TILE, TILE)

    size = (tile_rows * TILE, tile_cols * TILE)
    sums, pick = pl.pallas_call(
        functools.partial(count_kernel, n_row, n_col, ratio),
        out_shape=(
            jax.ShapeDtypeStruct((n_col, SECTIONS, TILE), jnp.int32), jax.ShapeDtypeStruct((1, TILE), jnp.int32)
        ),
        in_specs=[HBM, HBM],
        out_specs=(VMEM, VMEM),
        scratch_shapes=[
            pltpu.VMEM((SECTIONS, TILE), jnp.int32),
            pltpu.VMEM((ratio, panel, tile_cols), jnp.int32),
            pltpu.VMEM((n_col, n_row, SECTIONS, TILE), jnp.int32),
            pltpu.SMEM((SECTIONS,), jnp.int32), dma, dma, dma((n_row,)), dma((n_row,)), dma((n_col,)), dma((n_col,))
        ],
        compiler_params=pltpu.CompilerParams(
            collective_id=len(LENGTHS), has_side_effects=True, vmem_limit_bytes=8 * 1024 * 1024
        ),
        name="counts",
    )(in_hbm(sections), in_hbm(b_flags.reshape(ratio, panel, tile_cols)))

    def exchange(level, sections, a_flags, b_flags, a, b, sums):
        own_a, own_b, flags = pl.pallas_call(
            functools.partial(pack_kernel, tile_rows, panel, tile_cols, ratio),
            out_shape=(
                pltpu.VMEM(tiles(MOST), dtype),
                pltpu.VMEM(tiles(SECTIONS * MOST), dtype),
                pltpu.VMEM((1 + ratio, panel, TILE), jnp.int32),
            ),
            in_specs=[HBM] * 5,
            out_specs=(VMEM,) * 3,
            scratch_shapes=[
                pltpu.SMEM((SECTIONS,), jnp.int32),
                pltpu.SMEM((panel, tile_rows), jnp.int32),
                pltpu.SMEM(b_flags.shape, jnp.int32),
                pltpu.VMEM((panel, tile_rows), jnp.int32),
                pltpu.VMEM(b_flags.shape, jnp.int32),
                dma((5,)), dma,
            ],
            compiler_params=pltpu.CompilerParams(vmem_limit_bytes=16 * 1024 * 1024),
            name="pack",
        )(*[in_hbm(x) for x in (sections, a_flags, b_flags, a, b)])

        length = LENGTHS[level]
        chunks = length // SPAN
        handed = SPAN if level == 0 else max(2 * MOST - length, SPAN)
        done, meta = pl.pallas_call(
            functools.partial(comm_kernel, length, n_row, n_col, tile_rows, panel, tile_cols, ratio),
            out_shape=(
                pltpu.VMEM(size, dtype),
                pltpu.VMEM((tile_rows + 8, TILE), jnp.int32),
            ),
            in_specs=[HBM, VMEM, VMEM, VMEM, HBM],
            out_specs=(VMEM,) * 2,
            scratch_shapes=[
                pltpu.SMEM((SECTIONS,), jnp.int32),
                pltpu.SMEM((n_col, SECTIONS, TILE), jnp.int32),
                pltpu.VMEM((n_col, n_row, 1 + ratio, panel, TILE), jnp.int32),
                pltpu.VMEM((SECTIONS, 2, panel, TILE), jnp.int32),
                pltpu.SMEM((SECTIONS, 2, panel, TILE), jnp.int32),
                pltpu.SMEM((SECTIONS, 2, tile_rows), jnp.int32),
                pltpu.VMEM((n_row * tile_rows, TILE), jnp.float32),
                pltpu.VMEM(tiles(HALF), dtype),
                pltpu.VMEM(tiles(MOST), dtype),
                pltpu.VMEM(tiles(MOST), dtype),
                pltpu.VMEM(tiles(MOST), dtype),
                pltpu.VMEM(tiles(2 * MOST), dtype),
                pltpu.VMEM(tiles(2 * max(length - MOST, 1)), dtype),
                pltpu.VMEM(tiles(MOST), dtype),
                pltpu.VMEM(tiles(handed), dtype),
                pltpu.VMEM(tiles(handed), dtype),
                pltpu.VMEM(tiles(bits - 1, MOST), dtype),
                pltpu.VMEM(size if level else (8, TILE), jnp.float32),
                pltpu.VMEM((tile_rows * TILE, panel * TILE), dtype),
                pltpu.VMEM((panel * TILE, tile_cols * TILE), dtype),
                dma, dma, dma, dma, dma, dma((n_row,)), dma((n_row,)), dma((n_col,)), dma((n_col,)),
                dma((chunks,)), dma((chunks,)), dma((chunks,)), dma((chunks,)),
                dma((handed // SPAN,)), dma((handed // SPAN,)),
                dma, dma,
                dma((bits - 1, SECTIONS * A_STEPS)), dma((bits - 1, SECTIONS * A_STEPS)),
                dma((SECTIONS * A_STEPS,)), dma((SECTIONS * A_STEPS,)),
            ],
            compiler_params=pltpu.CompilerParams(
                collective_id=level, has_side_effects=True, vmem_limit_bytes=49 * 1024 * 1024
            ),
            name=f"exchange_{length}",
        )(in_hbm(sections), *[in_vmem(x) for x in (own_a, own_b, flags)], in_hbm(sums))

        return pl.pallas_call(
            functools.partial(final_kernel, tile_rows, tile_cols),
            out_shape=(jax.ShapeDtypeStruct(size, dtype), jax.ShapeDtypeStruct((tile_rows, tile_cols), jnp.int32)),
            in_specs=[VMEM] * 2,
            out_specs=(HBM, VMEM),
            scratch_shapes=[
                pltpu.SMEM(meta.shape, jnp.int32), pltpu.VMEM((TILE, TILE), dtype), dma, dma
            ],
            compiler_params=pltpu.CompilerParams(vmem_limit_bytes=12 * 1024 * 1024),
            name="compact",
        )(*[in_vmem(x) for x in (meta, done)])

    branches = [functools.partial(exchange, level) for level in range(len(LENGTHS))]
    return lax.switch(pick[0, 0], branches, sections, a_flags.T, b_flags, a_matrix, b_matrix, sums)


def solution(mesh):
    return jax.shard_map(
        functools.partial(shards, mesh.shape["row"], mesh.shape["col"]),
        mesh=mesh,
        in_specs=(P("row", "col"), P("row", "col"), P("row", "col"), P("row", "col"), P()),
        out_specs=(P("row", "col"), P("row", "col")),
        check_vma=False,
    )
```
